128 devices in a mesh: seq: 64 (over y, z, x), fsdp: 2 (over core).
Axes of the slice: x: 4, y: 4, z: 4, core: 2. Of those that a mesh axis runs over, the one named last changes fastest.
Arguments:
- tokens: bfloat16 [2, 49152, 2560], P('fsdp', 'seq'), may hold values from -6 to 6
- bounds: int32 [2, 64, 2], P('fsdp', 'seq'), may hold values from 0 to 96, as said below
- in_weight: bfloat16 [2560, 5416], P(('seq', 'fsdp')), may hold values from -0.125 to 0.125
- conv_weight: float32 [4, 2816], replicated, may hold values from -0.6 to 0.6
- conv_bias: float32 [2816], replicated, may hold values from -3 to 3
- dt_bias: float32 [40], replicated, may hold values from -4 to 0
- decay_rate: float32 [40], replicated, may hold values from 1.2207031e-05 to 0.5
- skip_gain: float32 [40], replicated, may hold values from 0.1 to 1.9
- norm_gain: float32 [2560], replicated, may hold values from 0.1 to 1.9
Outputs:
- layer_out: bfloat16 [2, 49152, 2560], P('fsdp', 'seq')
The draws below stay inside these ranges and needn't reach their ends.
Inputs may be any that keep to these rules, and one draw needn't show every extreme that they name: For sequence b, bounds[b, s] holds the first and one past the last block of the shard of index s of seq; shards are consecutive in s and cover all 96 blocks; each holds 1 to 3 blocks, and some shard holds 3.
All inputs are finite; a program needn't handle non-finite values.
Results may differ from the reference program's by a relative error of at most 0.0028.
The reference program's roundings to bfloat16 on the way count: a program that leaves them out, or rounds other values in their place, can miss the bound.
Values may be sent and summed in bfloat16 or wider, within the bound.
A program may use at most 192 MiB of HBM per device.

```python
import jax
import jax.numpy as jnp
from jax import lax

D = 2560
HEADS = 40
HEAD_DIM = 64
STATE = 128
CONV = 4
BLOCK = 256
SLOT_BLOCKS = 3
INNER = 2560
COLS = 5416
SLOTS = 768
TOTAL_BLOCKS = 96
SEQ_LEN = 24576
SEQS = 2
N_SEQ = 64


def draw_bounds(key, part):
    rows = []
    for index in range(SEQS):
        subkey = jax.random.fold_in(key, 11 + index)
        pick_key, order_key = jax.random.split(subkey)
        heavy = jax.random.randint(pick_key, (), 1, N_SEQ // 4 + 1)
        middle = N_SEQ // 2 - 2 * heavy
        ranking = jax.random.permutation(order_key, N_SEQ)
        counts = jnp.where(ranking < heavy, 3, jnp.where(ranking < heavy + middle, 2, 1)).astype(jnp.int32)
        ends = jnp.cumsum(counts).astype(jnp.int32)
        rows.append(jnp.stack([ends - counts, ends], axis=1))
    return jnp.stack(rows).astype(jnp.int32)


def draw_decay_rate(key, part):
    choose_key, value_key = jax.random.split(jax.random.fold_in(key, 5))
    slow_heads = jax.random.uniform(choose_key, (HEADS,)) < 0.5
    spread = jax.random.uniform(value_key, (HEADS,), jnp.float32)
    slow_rate = 0.3 / SEQ_LEN * jnp.exp(spread * jnp.log(10.0))
    fast_rate = 0.05 * jnp.exp(spread * jnp.log(10.0))
    return jnp.where(slow_heads, slow_rate, fast_rate).astype(jnp.float32)


def levels(rng, shape, shards, low, largest):
    gain = 1.0
    for position, shards_of in shards:
        draws = jax.random.uniform(jax.random.fold_in(jax.random.fold_in(rng, 6), position), (shards_of,), jnp.float32, low / len(shards), largest / len(shards))
        gain = gain * jnp.repeat(jnp.exp(draws), shape[position] // shards_of).reshape((-1,) + (1,) * (len(shape) - 1 - position))
    return gain


def noise(stream_key, shape, scale, limit, cuts=(), dtype=jnp.bfloat16):
    array = scale * jax.random.normal(stream_key, shape, jnp.float32)
    if cuts:
        array = array * levels(stream_key, shape, cuts, -0.22, 0.18)
    return jnp.clip(array, -limit, limit).astype(dtype)


def setup_inputs(seed: int = 0) -> dict:
    arg_keys = jax.random.split(jax.random.key(seed), 10)
    tokens = noise(arg_keys[0], (SEQS, N_SEQ * SLOTS, D), 1.0, 6.0, ((0, 2), (1, 64)))
    bounds = draw_bounds(jax.random.fold_in(arg_keys[9], 71), 0)
    in_weight = noise(arg_keys[2], (D, COLS), D ** -0.5, 0.125, ((0, 128),))
    conv_weight = jnp.clip(jax.random.uniform(arg_keys[3], (CONV, INNER + 2 * STATE), jnp.float32, -0.6, 0.6), -0.6, 0.6)
    conv_bias = noise(arg_keys[4], (INNER + 2 * STATE,), 0.5, 3.0, (), jnp.float32)
    dt_bias = jnp.clip(jax.random.uniform(arg_keys[5], (HEADS,), jnp.float32, -4.0, 0.0), -4.0, 0.0)
    decay_rate = draw_decay_rate(jax.random.fold_in(arg_keys[9], 71), 0)
    skip_gain = jnp.clip(1.0 + 0.18 * jax.random.normal(arg_keys[7], (HEADS,), jnp.float32), 0.1, 1.9)
    norm_gain = jnp.clip(1.0 + 0.18 * jax.random.normal(arg_keys[8], (INNER,), jnp.float32), 0.1, 1.9)
    return dict(tokens=tokens, bounds=bounds, in_weight=in_weight, conv_weight=conv_weight, conv_bias=conv_bias, dt_bias=dt_bias, decay_rate=decay_rate, skip_gain=skip_gain, norm_gain=norm_gain)


def block_terms(head_input, input_map, output_map, step_size, decay_rate):
    log_decay = -(step_size * decay_rate[None, :]).T
    cumulative = jnp.cumsum(log_decay, axis=1)
    pairwise = cumulative[:, :, None] - cumulative[:, None, :]
    length = cumulative.shape[1]
    causal = jnp.arange(length)[:, None] >= jnp.arange(length)[None, :]
    pair_decay = jnp.exp(jnp.where(causal[None], pairwise, -jnp.inf))
    scores = jnp.dot(output_map, input_map.T, preferred_element_type=jnp.float32)
    mixing = scores[None] * pair_decay * step_size.T[:, None, :]
    inner_out = jnp.einsum('hij,jhp->ihp', mixing, head_input, precision=lax.Precision.HIGH)
    to_end = jnp.exp(cumulative[:, -1:] - cumulative) * step_size.T
    local_state = jnp.einsum('hj,jhp,jn->hpn', to_end, head_input, input_map.astype(jnp.float32), precision=lax.Precision.HIGH)
    return (inner_out, cumulative, local_state)

def carried(output_map, cumulative, state):
    reach = jnp.einsum('in,hpn->ihp', output_map.astype(jnp.float32), state, precision=lax.Precision.HIGH)
    return jnp.exp(cumulative).T[:, :, None] * reach

def one_sequence(tokens, bounds, in_weight, conv_weight, conv_bias, dt_bias, decay_rate, skip_gain, norm_gain):
    starts = bounds[:, 0]
    ends = bounds[:, 1]
    blocks = jnp.arange(TOTAL_BLOCKS).astype(jnp.int32)
    owner = lax.optimization_barrier(jnp.sum((ends[None, :] <= blocks[:, None]).astype(jnp.int32), axis=1)).astype(jnp.int32)
    slot_row = (owner * SLOT_BLOCKS + blocks - starts[owner]).astype(jnp.int32)
    grouped = tokens.reshape(N_SEQ * SLOT_BLOCKS, BLOCK, D)
    live = grouped[slot_row].reshape(SEQ_LEN, D)
    projected = jnp.dot(live, in_weight, preferred_element_type=jnp.float32).astype(jnp.bfloat16)
    gate = projected[:, :INNER].astype(jnp.float32)
    mixed_in = projected[:, INNER:2 * INNER + 2 * STATE]
    raw_step = projected[:, 2 * INNER + 2 * STATE:].astype(jnp.float32)
    padded = jnp.concatenate([jnp.zeros((CONV - 1, mixed_in.shape[1]), jnp.bfloat16), mixed_in], axis=0)
    convolved = jnp.zeros((SEQ_LEN, mixed_in.shape[1]), jnp.float32) + conv_bias[None, :]
    for offset in range(CONV):
        convolved = convolved + conv_weight[offset][None, :] * padded[offset:offset + SEQ_LEN].astype(jnp.float32)
    conv_out = jax.nn.silu(convolved).astype(jnp.bfloat16)
    head_input = conv_out[:, :INNER].astype(jnp.float32).reshape(TOTAL_BLOCKS, BLOCK, HEADS, HEAD_DIM)
    input_map = conv_out[:, INNER:INNER + STATE].reshape(TOTAL_BLOCKS, BLOCK, STATE)
    output_map = conv_out[:, INNER + STATE:].reshape(TOTAL_BLOCKS, BLOCK, STATE)
    step_size = jax.nn.softplus(raw_step + dt_bias[None, :]).reshape(TOTAL_BLOCKS, BLOCK, HEADS)

    def advance(state, pieces):
        in_values, in_map, out_map, in_step = pieces
        inner_out, cumulative, local_state = block_terms(in_values, in_map, out_map, in_step, decay_rate)
        result = inner_out + carried(out_map, cumulative, state) + skip_gain[None, :, None] * in_values
        state = jnp.exp(cumulative[:, -1])[:, None, None] * state + local_state
        return (state, result)
    initial = jnp.zeros((HEADS, HEAD_DIM, STATE), jnp.float32)
    final_state, outputs = lax.scan(advance, initial, (head_input, input_map, output_map, step_size))
    scanned = outputs.reshape(SEQ_LEN, INNER)
    gated = scanned * jax.nn.silu(gate)
    normed = gated * lax.rsqrt(lax.optimization_barrier(jnp.mean(gated * gated, axis=1, keepdims=True)) + 1e-05) * norm_gain[None, :]
    placed = jnp.zeros((N_SEQ * SLOT_BLOCKS, BLOCK, INNER), jnp.bfloat16)
    placed = placed.at[slot_row].set(normed.astype(jnp.bfloat16).reshape(TOTAL_BLOCKS, BLOCK, INNER))
    return placed.reshape(N_SEQ * SLOTS, INNER)

def reference(tokens, bounds, in_weight, conv_weight, conv_bias, dt_bias, decay_rate, skip_gain, norm_gain):
    results = [one_sequence(tokens[index], bounds[index], in_weight, conv_weight, conv_bias, dt_bias, decay_rate, skip_gain, norm_gain) for index in range(SEQS)]
    return jnp.stack(results)
```

```python
import functools

import jax
import jax.numpy as jnp
from jax import lax
from jax.experimental import pallas as pl
from jax.experimental.pallas import tpu as pltpu
from jax.sharding import Mesh
from jax.sharding import PartitionSpec as P

BLOCK = 256
CHUNK = 128
HALO = 16
LANES = 128
LOG2E = 1.4426950408889634
AXES = ("y", "z", "xh", "xl")
F32 = jnp.float32
BF16 = jnp.bfloat16
MESH = pl.DeviceIdType.MESH
ORDERS = (("x", "y", "z"), ("y", "z", "x"), ("z", "x", "y"))


def split3(value):
    hi = value.astype(BF16)
    rest = value - hi.astype(F32)
    mid = rest.astype(BF16)
    lo = (rest - mid.astype(F32)).astype(BF16)
    return hi, mid, lo


def split2(value):
    hi = value.astype(BF16)
    lo = (value - hi.astype(F32)).astype(BF16)
    return hi, lo


def dot(a, b):
    return jnp.dot(a, b, preferred_element_type=F32)


def place():
    return {
        "y": lax.axis_index("y"),
        "z": lax.axis_index("z"),
        "x": lax.axis_index("xh") * 2 + lax.axis_index("xl"),
    }


def device_of(axis, coordinate):
    if axis == "x":
        return {"xh": coordinate // 2, "xl": lax.rem(coordinate, 2)}
    return {axis: coordinate}


def gather_kernel(block_ref, out_ref, local_sem, send_sem, recv_sem):
    me = place()
    near = lambda axis, step: lax.rem(me[axis] + step + 4, 4)
    barrier = pltpu.get_barrier_semaphore()
    for axis in ("y", "z", "x"):
        for step in (1, -1):
            pl.semaphore_signal(
                barrier, inc=1, device_id=device_of(axis, near(axis, step)), device_id_type=MESH
            )
    pl.semaphore_wait(barrier, 6)
    width = block_ref.shape[1] // 6

    def region(color, half, where):
        y, z, x = (where[axis] for axis in ("y", "z", "x"))
        xl, xh = (slice(None), slice(None)) if x is None else (lax.rem(x, 2), x // 2)
        y = slice(None) if y is None else y
        z = slice(None) if z is None else z
        return out_ref.at[xl, y, z, xh, :, pl.ds((color * 2 + half) * width, width)]

    own = pltpu.make_async_copy(
        block_ref, out_ref.at[lax.rem(me["x"], 2), me["y"], me["z"], me["x"] // 2], local_sem
    )
    own.start()

    def where(color, stage, coordinate):
        order = ORDERS[color]
        spot = dict(me)
        for axis in order[:stage]:
            spot[axis] = None
        spot[order[stage]] = coordinate
        return spot

    SLOTS = ((0, 0, 1), (0, 1, 1), (-1, 0, 1), (0, 1, -1), (0, 0, -1), (1, 1, -1))

    def copy(color, stage, slot):
        offset, half, step = SLOTS[slot]
        axis = ORDERS[color][stage]
        target = region(color, half, where(color, stage, near(axis, offset)))
        source = target
        if stage == 0 and offset == 0:
            source = block_ref.at[:, pl.ds((color * 2 + half) * width, width)]
        return pltpu.make_async_remote_copy(
            src_ref=source,
            dst_ref=target,
            send_sem=send_sem.at[color, stage, slot],
            recv_sem=recv_sem.at[color, stage, slot],
            device_id=device_of(axis, near(axis, step)),
            device_id_type=MESH,
        )

    def arrival(color, stage, slot):
        offset, half, step = SLOTS[slot]
        axis = ORDERS[color][stage]
        target = region(color, half, where(color, stage, near(axis, offset - step)))
        return pltpu.make_async_remote_copy(
            src_ref=target,
            dst_ref=target,
            send_sem=send_sem.at[color, stage, slot],
            recv_sem=recv_sem.at[color, stage, slot],
            device_id=device_of(axis, near(axis, step)),
            device_id_type=MESH,
        )

    for stage in range(3):
        for color in range(3):
            if stage:
                for slot in (1, 2, 4, 5):
                    arrival(color, stage - 1, slot).wait_recv()
                if stage == 1 and color == 0:
                    own.wait()
            for slot in (0, 3, 1, 4):
                copy(color, stage, slot).start()
        for color in range(3):
            arrival(color, stage, 0).wait_recv()
            copy(color, stage, 2).start()
            arrival(color, stage, 3).wait_recv()
            copy(color, stage, 5).start()
    for color in range(3):
        for slot in (1, 2, 4, 5):
            arrival(color, 2, slot).wait_recv()
    for stage in range(3):
        for color in range(3):
            for slot in range(6):
                copy(color, stage, slot).wait_send()


def gather_weight(block):
    rows, columns = block.shape
    return pl.pallas_call(
        gather_kernel,
        out_shape=jax.ShapeDtypeStruct((2, 4, 4, 2, rows, columns), BF16),
        in_specs=[pl.BlockSpec(memory_space=pltpu.VMEM)],
        out_specs=pl.BlockSpec(memory_space=pl.ANY),
        scratch_shapes=[
            pltpu.SemaphoreType.DMA,
            pltpu.SemaphoreType.DMA((3, 3, 6)),
            pltpu.SemaphoreType.DMA((3, 3, 6)),
        ],
        compiler_params=pltpu.CompilerParams(collective_id=0, has_side_effects=True),
        name="weight_gather",
    )(block)


def scan_kernel(
    live_ref, mixed_ref, raw_ref, taps_ref, bias_ref, dt_ref, decay_ref, skip_ref, spread_ref,
    tri_ref, y_ref, map_ref, cum_ref, state_ref, total_ref,
):
    inner = skip_ref.shape[1]
    state_width = (mixed_ref.shape[2] - inner) // 2
    chunk = pl.program_id(1)
    row0 = pl.multiple_of(chunk * CHUNK, CHUNK)

    @pl.when(chunk == 0)
    def _():
        state_ref[...] = jnp.zeros_like(state_ref)
        total_ref[...] = jnp.zeros_like(total_ref)

    mixed = mixed_ref[0, pl.ds(row0, CHUNK + HALO), :].astype(F32)
    taps = taps_ref.shape[0]
    conv = bias_ref[...] + taps_ref[0:1, :] * mixed[HALO - taps + 1 : HALO - taps + 1 + CHUNK]
    for k in range(1, taps):
        start = HALO - taps + 1 + k
        conv = conv + taps_ref[k : k + 1, :] * mixed[start : start + CHUNK]
    act = (conv * jax.nn.sigmoid(conv)).astype(BF16)
    x = act[:, :inner]
    in_map = act[:, inner : inner + state_width]
    out_map = act[:, inner + state_width :]

    raw = raw_ref[0, pl.ds(row0 + HALO, CHUNK), :].astype(F32) + dt_ref[...]
    tail = jnp.exp(-jnp.abs(raw))
    log1p = jnp.where(
        tail < 0.01, tail * (1.0 - tail * (0.5 - tail * (1.0 / 3.0 - 0.25 * tail))), jnp.log(1.0 + tail)
    )
    step = jnp.maximum(raw, 0.0) + log1p
    rows = lax.broadcasted_iota(jnp.int32, (CHUNK, LANES), 0)
    columns = lax.broadcasted_iota(jnp.int32, (CHUNK, LANES), 1)
    step = jnp.where(rows + row0 < live_ref[pl.program_id(0)], step, 0.0)
    log_decay = -(step * decay_ref[...]) * LOG2E
    cum = dot(tri_ref[...], jnp.concatenate(split3(log_decay), axis=0))
    shifted = jnp.where(step > 0.0, cum - jnp.log(step) * LOG2E, 1e30).T
    causal = rows >= columns
    scores = lax.dot_general(out_map, in_map, (((1,), (1,)), ((), ())), preferred_element_type=F32)

    state = state_ref[0]
    growth = dot(jnp.concatenate(split3(jnp.exp2(cum)), axis=1), spread_ref[...])
    reach = dot(
        jnp.concatenate([out_map, out_map], axis=1), jnp.concatenate(split2(state), axis=0)
    )
    base = growth * reach + skip_ref[...] * x.astype(F32)
    left = columns < LANES // 2
    zero = jnp.zeros((CHUNK, LANES), BF16)
    for tile in range(inner // LANES):
        lanes = slice(tile * LANES, (tile + 1) * LANES)
        total = base[:, lanes]
        for part in range(2):
            head = tile * 2 + part
            reached = jnp.where(
                causal, cum[:, head : head + 1] - shifted[head : head + 1, :], -1e30
            )
            mixing = jnp.exp2(reached) * scores
            values = jnp.where(left if part == 0 else ~left, x[:, lanes], zero)
            total = total + dot(
                jnp.concatenate(split2(mixing), axis=1), jnp.concatenate([values, values], axis=0)
            )
        y_ref[0, :, lanes] = total

    last = cum[CHUNK - 1 : CHUNK, :]
    to_end = jnp.exp2(last - cum) * step
    weighted = x.astype(F32) * dot(jnp.concatenate(split3(to_end), axis=1), spread_ref[...])
    added = lax.dot_general(
        jnp.concatenate([in_map, in_map], axis=0),
        jnp.concatenate(split2(weighted), axis=0),
        (((0,), (0,)), ((), ())),
        preferred_element_type=F32,
    )
    state_ref[0] = growth[CHUNK - 1 : CHUNK, :] * state + added
    map_ref[0] = out_map
    cum_ref[0] = cum + total_ref[0]
    total_ref[0] = total_ref[0] + last


def scan_call(live, mixed, raw, taps, bias, dt, decay, skip, spread, tri):
    seqs, padded, width = mixed.shape
    slots = padded - HALO
    inner = skip.shape[1]
    state_width = (width - inner) // 2
    chunks = slots // CHUNK
    whole = lambda a: pl.BlockSpec(a.shape, lambda q, c: (0,) * a.ndim)
    return pl.pallas_call(
        scan_kernel,
        grid=(seqs, chunks),
        in_specs=[
            pl.BlockSpec(memory_space=pltpu.SMEM),
            pl.BlockSpec((1, padded, width), lambda q, c: (q, 0, 0)),
            pl.BlockSpec((1, padded, LANES), lambda q, c: (q, 0, 0)),
            whole(taps), whole(bias), whole(dt), whole(decay), whole(skip), whole(spread), whole(tri),
        ],
        out_specs=[
            pl.BlockSpec((1, CHUNK, inner), lambda q, c: (q, c, 0)),
            pl.BlockSpec((1, CHUNK, state_width), lambda q, c: (q, c, 0)),
            pl.BlockSpec((1, CHUNK, LANES), lambda q, c: (q, c, 0)),
            pl.BlockSpec((1, state_width, inner), lambda q, c: (q, 0, 0)),
            pl.BlockSpec((1, 1, LANES), lambda q, c: (q, 0, 0)),
        ],
        out_shape=[
            jax.ShapeDtypeStruct((seqs, slots, inner), F32),
            jax.ShapeDtypeStruct((seqs, slots, state_width), BF16),
            jax.ShapeDtypeStruct((seqs, slots, LANES), F32),
            jax.ShapeDtypeStruct((seqs, state_width, inner), F32),
            jax.ShapeDtypeStruct((seqs, 1, LANES), F32),
        ],
        compiler_params=pltpu.CompilerParams(
            dimension_semantics=("arbitrary", "arbitrary"), vmem_limit_bytes=50 * 1024 * 1024
        ),
        name="conv_scan",
    )(live, mixed, raw, taps, bias, dt, decay, skip, spread, tri)


def prefix_kernel(
    state_ref, total_ref, spread_ref, in_ref, decays, pieces, arrived, starts, factors,
    send_sem, recv_sem, dsend_sem, drecv_sem, bsend_sem, brecv_sem,
):
    count = 64
    y, z, xh, xl = (lax.axis_index(axis) for axis in AXES)
    me = ((y * 4 + z) * 2 + xh) * 2 + xl
    inner = state_ref.shape[2]
    wide = inner // 2

    def device(index):
        return {
            "y": index // 16,
            "z": lax.rem(index // 4, 4),
            "xh": lax.rem(index // 2, 2),
            "xl": lax.rem(index, 2),
        }

    def slice_of(ref, index):
        row = pl.multiple_of(lax.rem(index // 2, 16) * 8, 8)
        column = pl.multiple_of(lax.rem(index, 2) * wide, LANES)
        return ref.at[index // 32, pl.ds(row, 8), pl.ds(column, wide)]

    barrier = pltpu.get_barrier_semaphore()

    @pl.loop(1, count)
    def _(i):
        pl.semaphore_signal(
            barrier, inc=1, device_id=device(lax.rem(me + i, count)), device_id_type=MESH
        )

    pl.semaphore_wait(barrier, count - 1)
    decays[...] = jnp.exp2(total_ref[...])

    def piece(index, slot):
        return pltpu.make_async_remote_copy(
            src_ref=slice_of(state_ref, index), dst_ref=arrived.at[slot],
            send_sem=send_sem.at[index], recv_sem=recv_sem.at[slot],
            device_id=device(index), device_id_type=MESH,
        )

    def factor(index, slot):
        return pltpu.make_async_remote_copy(
            src_ref=total_ref.at[index // 32], dst_ref=pieces.at[slot],
            send_sem=dsend_sem.at[index], recv_sem=drecv_sem.at[slot],
            device_id=device(index), device_id_type=MESH,
        )

    def back(index, slot):
        return pltpu.make_async_remote_copy(
            src_ref=starts.at[index], dst_ref=slice_of(in_ref, slot),
            send_sem=bsend_sem.at[index], recv_sem=brecv_sem.at[slot],
            device_id=device(index), device_id_type=MESH,
        )

    @pl.loop(1, count)
    def _(i):
        peer = lax.rem(me + i, count)
        factor(peer, me).start()
        piece(peer, me).start()

    arrived[me] = slice_of(state_ref, me)[...]
    pieces[me] = total_ref[me // 32]

    @pl.loop(1, count)
    def _(i):
        peer = lax.rem(me + i, count)
        factor(peer, peer).wait_recv()

    column = pl.multiple_of(lax.rem(me, 2) * wide, LANES)
    decay = jnp.exp2(pieces[...].reshape(count, LANES))
    factors[...] = dot(
        jnp.concatenate(split3(decay), axis=1), spread_ref[:, pl.ds(column, wide)]
    )

    @pl.loop(1, count)
    def _(i):
        peer = lax.rem(me + i, count)
        piece(peer, peer).wait_recv()

    def compose(index, carry):
        starts[index] = carry
        return factors[pl.ds(index, 1), :] * carry + arrived[index]

    lax.fori_loop(0, count, compose, jnp.zeros((8, wide), F32))

    @pl.loop(1, count)
    def _(i):
        back(lax.rem(me + i, count), me).start()

    slice_of(in_ref, me)[...] = starts[me]

    @pl.loop(1, count)
    def _(i):
        peer = lax.rem(me + i, count)
        back(peer, peer).wait_recv()

    @pl.loop(1, count)
    def _(i):
        peer = lax.rem(me + i, count)
        piece(peer, me).wait_send()
        factor(peer, me).wait_send()
        back(peer, me).wait_send()


def prefix_call(state, total, spread):
    seqs, state_width, inner = state.shape
    wide = inner // 2
    return pl.pallas_call(
        prefix_kernel,
        out_shape=jax.ShapeDtypeStruct(state.shape, F32),
        in_specs=[pl.BlockSpec(memory_space=pltpu.VMEM)] * 3,
        out_specs=pl.BlockSpec(memory_space=pltpu.VMEM),
        scratch_shapes=[
            pltpu.VMEM((seqs, 1, LANES), F32),
            pltpu.VMEM((64, 1, LANES), F32),
            pltpu.VMEM((64, 8, wide), F32),
            pltpu.VMEM((64, 8, wide), F32),
            pltpu.VMEM((64, wide), F32),
        ]
        + [pltpu.SemaphoreType.DMA((64,))] * 6,
        compiler_params=pltpu.CompilerParams(collective_id=1, has_side_effects=True),
        name="state_prefix",
    )(state, total, spread)


def gated_kernel(y_ref, map_ref, cum_ref, gate_ref, start_ref, spread_ref, out_ref, square_ref):
    growth = dot(jnp.concatenate(split3(jnp.exp2(cum_ref[0])), axis=1), spread_ref[...])
    out_map = map_ref[0]
    reach = dot(
        jnp.concatenate([out_map, out_map], axis=1),
        jnp.concatenate(split2(start_ref[0]), axis=0),
    )
    row0 = pl.multiple_of(pl.program_id(1) * CHUNK, CHUNK)
    gate = gate_ref[0, pl.ds(row0 + HALO, CHUNK), :].astype(F32)
    gated = (y_ref[0] + growth * reach) * (gate * jax.nn.sigmoid(gate))
    out_ref[0] = gated
    square_ref[0] = jnp.broadcast_to(jnp.sum(gated * gated, axis=1, keepdims=True), (CHUNK, LANES))


def gated_call(y, out_map, cum, gate, start, spread):
    seqs, slots, inner = y.shape
    state_width = out_map.shape[2]
    padded = gate.shape[1]
    return pl.pallas_call(
        gated_kernel,
        grid=(seqs, slots // CHUNK),
        in_specs=[
            pl.BlockSpec((1, CHUNK, inner), lambda q, c: (q, c, 0)),
            pl.BlockSpec((1, CHUNK, state_width), lambda q, c: (q, c, 0)),
            pl.BlockSpec((1, CHUNK, LANES), lambda q, c: (q, c, 0)),
            pl.BlockSpec((1, padded, inner), lambda q, c: (q, 0, 0)),
            pl.BlockSpec((1, state_width, inner), lambda q, c: (q, 0, 0)),
            pl.BlockSpec(spread.shape, lambda q, c: (0, 0)),
        ],
        out_specs=[
            pl.BlockSpec((1, CHUNK, inner), lambda q, c: (q, c, 0)),
            pl.BlockSpec((1, CHUNK, LANES), lambda q, c: (q, c, 0)),
        ],
        out_shape=[
            jax.ShapeDtypeStruct((seqs, slots, inner), F32),
            jax.ShapeDtypeStruct((seqs, slots, LANES), F32),
        ],
        compiler_params=pltpu.CompilerParams(dimension_semantics=("arbitrary", "arbitrary")),
        name="gated",
    )(y, out_map, cum, gate, start, spread)


def local(
    tokens, bounds, in_weight, conv_weight, conv_bias, dt_bias, decay_rate, skip_gain, norm_gain
):
    slots, model = tokens.shape[1:]
    width = norm_gain.shape[0]
    inner = width // 2
    state_width = (conv_bias.shape[0] - width) // 2
    heads = decay_rate.shape[0] // 2
    core = lax.axis_index("core")
    swap = [(0, 1), (1, 0)]

    def half(array, start, size):
        low = array[..., start : start + size]
        return jnp.where(core == 0, low, array[..., start + size : start + 2 * size])

    rows = lax.all_gather(in_weight, ("xl", "core"), axis=0, tiled=True)
    first = jnp.concatenate(
        [half(rows, width, inner), rows[:, 2 * width : 2 * width + 2 * state_width]], axis=1
    )
    raw = half(rows, 2 * width + 2 * state_width, heads)
    second = jnp.concatenate(
        [
            jnp.pad(raw, ((0, 0), (0, LANES - heads))),
            half(rows, 0, inner),
            jnp.zeros((rows.shape[0], first.shape[1] - inner - LANES), BF16),
        ],
        axis=1,
    )
    block = jnp.where(lax.axis_index("xl") == 0, first, second)
    weight = gather_weight(block).reshape(2, model, first.shape[1])

    blocks = bounds[0, 0, 1] - bounds[0, 0, 0]
    edge = lax.dynamic_slice_in_dim(tokens[0], blocks * BLOCK - HALO, HALO, 0)
    edge = lax.ppermute(edge, AXES, [(s, s + 1) for s in range(63)])
    mark = jnp.where(jnp.arange(HALO)[:, None] == 0, blocks.astype(BF16), edge)
    extended = jnp.concatenate([mark, tokens[0]], axis=0)
    other = lax.ppermute(extended, "core", swap)
    live = jnp.stack([blocks, other[0, 0].astype(jnp.int32)]) * BLOCK
    rows_in = jnp.concatenate([extended, other], axis=0)
    mixed = dot(rows_in, weight[0]).astype(BF16).reshape(2, slots + HALO, -1)
    rest = dot(rows_in, weight[1]).astype(BF16).reshape(2, slots + HALO, -1)

    spread = (jnp.arange(inner)[None, :] // (inner // heads) == jnp.arange(LANES)[:, None]).astype(BF16)
    spread = jnp.concatenate([spread] * 3, axis=0)
    tri = (jnp.arange(CHUNK)[:, None] >= jnp.arange(CHUNK)[None, :]).astype(BF16)
    tri = jnp.concatenate([tri] * 3, axis=1)
    own_columns = lambda a: jnp.concatenate([half(a, 0, inner), a[..., width:]], axis=-1)
    per_head = lambda a: jnp.pad(half(a, 0, heads), (0, LANES - heads))[None]
    skip = jnp.repeat(half(skip_gain, 0, heads), inner // heads)[None]
    y, out_map, cum, state, total = scan_call(
        live, mixed, rest[:, :, :LANES], own_columns(conv_weight), own_columns(conv_bias)[None],
        per_head(dt_bias), per_head(decay_rate), skip, spread, tri,
    )
    start = prefix_call(state, total, spread)
    gated, square = gated_call(y, out_map, cum, rest[:, :, LANES : LANES + inner], start, spread)
    square = square[:, :, :1]
    square = square + lax.ppermute(square[::-1], "core", swap)
    normed = gated * lax.rsqrt(square / width + 1e-05) * half(norm_gain, 0, inner)[None, None]
    normed = normed.astype(BF16)
    far = lax.ppermute(normed[1], "core", swap)
    near = normed[0]
    out = jnp.where(
        core == 0, jnp.concatenate([near, far], axis=1), jnp.concatenate([far, near], axis=1)
    )
    out = jnp.where(jnp.arange(slots)[:, None] < live[0], out, jnp.zeros_like(out))
    return out[None]


def solution(mesh):
    split = Mesh(mesh.devices.reshape(4, 4, 2, 2, 2), AXES + ("core",))
    return jax.shard_map(
        local,
        mesh=split,
        in_specs=(
            P("core", AXES, None),
            P("core", AXES, None),
            P(AXES + ("core",), None),
            P(), P(), P(), P(), P(), P(),
        ),
        out_specs=P("core", AXES, None),
        check_vma=False,
    )
```

```python
import jax
import jax.numpy as jnp
import numpy as np
from jax import lax
from jax.experimental import pallas as pl
from jax.experimental.pallas import tpu as pltpu
from jax.sharding import Mesh
from jax.sharding import PartitionSpec as P

BLOCK = 256
CHUNK = 128
HALO = 16
LANES = 128
COUNT = 64
OWNERS = 32
LOG2E = 1.4426950408889634
AXES = ("y", "z", "xh", "xl")
F32 = jnp.float32
BF16 = jnp.bfloat16
MESH = pl.DeviceIdType.MESH
ORDERS = (("x", "y", "z"), ("y", "z", "x"), ("z", "x", "y"))
SLOTS = ((0, 0, 1), (0, 1, 1), (-1, 0, 1), (0, 1, -1), (0, 0, -1), (1, 1, -1))


def split3(value):
    hi = value.astype(BF16)
    rest = value - hi.astype(F32)
    mid = rest.astype(BF16)
    lo = (rest - mid.astype(F32)).astype(BF16)
    return hi, mid, lo


def split2(value):
    hi = value.astype(BF16)
    lo = (value - hi.astype(F32)).astype(BF16)
    return hi, lo


def dot(a, b):
    return jnp.dot(a, b, preferred_element_type=F32)


def layer_kernel(
    live_ref, edge_ref, tokens_ref, pieces_ref, params_ref, heads_ref, spread_ref, tri_ref,
    out_ref,
    rows_in, weight, proj, far_map, y_all, map_all, cum_all, state, total, parts, block, arrived,
    starts, decays, factors, incoming, square, far_square, staged, live,
    part_send, part_recv, token_sem, token_send, token_recv, edge_send, edge_recv, live_send,
    live_recv, gather_send, gather_recv, map_send, map_recv, piece_send, piece_recv, decay_send,
    decay_recv, back_send, back_recv, square_send, square_recv, out_send, out_recv,
):
    y, z, xh, xl = (lax.axis_index(axis) for axis in AXES)
    core = lax.axis_index("core")
    x = xh * 2 + xl
    here = {"y": y, "z": z, "x": x}
    me = (y * 4 + z) * 4 + x
    slots, model = tokens_ref.shape
    inner = model // 2
    wide = inner // 2
    group_width = weight.shape[-1]
    partner = {"core": 1 - core}
    core_lane = pl.multiple_of(core * inner, LANES)

    def device(index):
        return {
            "y": index // 16,
            "z": lax.rem(index // 4, 4),
            "xh": lax.rem(index // 2, 2),
            "xl": lax.rem(index, 2),
        }

    def remote(source, target, send, recv, where):
        return pltpu.make_async_remote_copy(
            src_ref=source, dst_ref=target, send_sem=send, recv_sem=recv,
            device_id=where, device_id_type=MESH,
        )

    barrier = pltpu.get_barrier_semaphore()

    @pl.loop(1, 2 * COUNT)
    def _(i):
        other = lax.rem(me * 2 + core + i, 2 * COUNT)
        pl.semaphore_signal(
            barrier, inc=1, device_id={**device(other // 2), "core": lax.rem(other, 2)},
            device_id_type=MESH,
        )

    pl.semaphore_wait(barrier, 2 * COUNT - 1)

    my_part = xl * 2 + core

    def part_copy(step):
        target = lax.rem(my_part + step, 4)
        return remote(
            pieces_ref.at[target], parts.at[my_part], part_send.at[step], part_recv.at[step],
            {"xl": target // 2, "core": lax.rem(target, 2)},
        )

    def part_arrival(step):
        source = lax.rem(my_part + 4 - step, 4)
        return remote(
            pieces_ref.at[0], parts.at[source], part_send.at[step], part_recv.at[step], partner
        )

    for step in (1, 2, 3):
        part_copy(step).start()
    parts[my_part] = pieces_ref[my_part]

    own_rows = pltpu.make_async_copy(tokens_ref, rows_in.at[core, pl.ds(HALO, slots)], token_sem)
    own_rows.start()
    rows_copy = remote(
        tokens_ref, rows_in.at[core, pl.ds(HALO, slots)], token_send, token_recv, partner
    )
    live[core] = live_ref[...]
    live_copy = remote(live_ref, live.at[core], live_send, live_recv, partner)
    live_copy.start()

    def edge_copy(side):
        return remote(
            edge_ref, rows_in.at[core, pl.ds(0, HALO)], edge_send.at[side], edge_recv.at[core],
            {**device(me + 1), "core": side},
        )

    @pl.when(me < COUNT - 1)
    def _():
        for side in range(2):
            edge_copy(side).start()

    @pl.when(me == 0)
    def _():
        rows_in[:, 0:HALO, :] = jnp.zeros((2, HALO, model), BF16)

    for step in (1, 2, 3):
        part_arrival(step).wait_recv()
    block[...] = jnp.concatenate([parts[i].astype(F32) for i in range(4)], axis=0).astype(BF16)

    near = lambda axis, step: lax.rem(here[axis] + step + 4, 4)
    unit = group_width // 6

    def along(axis, step):
        coordinate = near(axis, step)
        if axis == "x":
            return {"xh": coordinate // 2, "xl": lax.rem(coordinate, 2)}
        return {axis: coordinate}

    def region(group, color, half, spot):
        wy, wz, wx = (spot[axis] for axis in ("y", "z", "x"))
        low, high = (slice(None), slice(None)) if wx is None else (lax.rem(wx, 2), wx // 2)
        wy = slice(None) if wy is None else wy
        wz = slice(None) if wz is None else wz
        return weight.at[group, low, wy, wz, high, :, pl.ds((color * 2 + half) * unit, unit)]

    def spot_of(color, stage, coordinate):
        spot = dict(here)
        for axis in ORDERS[color][:stage]:
            spot[axis] = None
        spot[ORDERS[color][stage]] = coordinate
        return spot

    def ring_copy(group, color, stage, slot):
        offset, half, step = SLOTS[slot]
        axis = ORDERS[color][stage]
        target = region(group, color, half, spot_of(color, stage, near(axis, offset)))
        source = target
        if stage == 0 and offset == 0:
            source = block.at[:, pl.ds(group * group_width + (color * 2 + half) * unit, unit)]
        return remote(
            source, target, gather_send.at[group, color, stage, slot],
            gather_recv.at[group, color, stage, slot], along(axis, step),
        )

    def ring_arrival(group, color, stage, slot):
        offset, half, step = SLOTS[slot]
        axis = ORDERS[color][stage]
        target = region(group, color, half, spot_of(color, stage, near(axis, offset - step)))
        return remote(
            target, target, gather_send.at[group, color, stage, slot],
            gather_recv.at[group, color, stage, slot], along(axis, step),
        )

    def ring_start(group, stage):
        for color in range(3):
            if stage:
                for slot in (1, 2, 4, 5):
                    ring_arrival(group, color, stage - 1, slot).wait_recv()
            for slot in (0, 3, 1, 4):
                ring_copy(group, color, stage, slot).start()

    def ring_forward(group, stage):
        for color in range(3):
            ring_arrival(group, color, stage, 0).wait_recv()
            ring_copy(group, color, stage, 2).start()
            ring_arrival(group, color, stage, 3).wait_recv()
            ring_copy(group, color, stage, 5).start()

    def ring_finish(group):
        for color in range(3):
            for slot in (1, 2, 4, 5):
                ring_arrival(group, color, 2, slot).wait_recv()

    ring_start(0, 0)
    rows_copy.start()
    for group in range(2):
        weight[group, xl, y, z, xh] = block[:, group * group_width : (group + 1) * group_width]
    ring_forward(0, 0)
    ring_start(0, 1)
    ring_start(1, 0)
    ring_forward(0, 1)
    ring_forward(1, 0)
    ring_start(0, 2)
    ring_forward(0, 2)
    ring_start(1, 1)
    own_rows.wait()
    rows_copy.wait_send()
    remote(
        tokens_ref, rows_in.at[1 - core, pl.ds(HALO, slots)], token_send, token_recv, partner
    ).wait_recv()
    remote(live_ref, live.at[1 - core], live_send, live_recv, partner).wait_recv()

    @pl.when(me > 0)
    def _():
        for side in range(2):
            remote(
                edge_ref, rows_in.at[side, pl.ds(0, HALO)], edge_send.at[side], edge_recv.at[side],
                partner,
            ).wait_recv()

    ring_finish(0)

    def project(group, first, last):
        @pl.loop(first, last)
        def _(i):
            seq = lax.rem(i, 2)
            tile = i // 2
            columns = pl.ds(pl.multiple_of(lax.rem(tile, 3) * 2 * LANES, LANES), 2 * LANES)
            matrix = weight[group, tile // 3, :, :, :, :, columns].reshape(model, 2 * LANES)
            proj[seq, :, pl.ds(pl.multiple_of(tile * 2 * LANES, LANES), 2 * LANES)] = dot(
                rows_in[seq], matrix
            ).astype(BF16)

    map_copy = remote(proj.at[:, :, pl.ds(0, LANES)], far_map, map_send, map_recv, partner)
    project(0, 0, 4)
    map_copy.start()
    ring_forward(1, 1)
    project(0, 4, 8)
    ring_start(1, 2)
    project(0, 8, 12)
    map_copy.wait()

    def slice_of(ref, seq, k):
        row = pl.multiple_of(k // 2 * 8, 8)
        column = pl.multiple_of(lax.rem(k, 2) * wide, LANES)
        return ref.at[seq, pl.ds(row, 8), pl.ds(column, wide)]

    my_k = (y * 4 + z) * 2 + xh
    my_seq = lax.rem(y + z + xl, 2)

    def owner(seq, k):
        oy, oz = k // 8, lax.rem(k // 2, 4)
        return {"y": oy, "z": oz, "xh": lax.rem(k, 2), "xl": lax.rem(seq + oy + oz, 2)}

    def piece(seq, k, slot):
        return remote(
            slice_of(state, seq, k), arrived.at[slot], piece_send.at[seq * OWNERS + k],
            piece_recv.at[slot], owner(seq, k),
        )

    def decay_copy(seq, k, slot):
        return remote(
            total.at[seq], decays.at[slot], decay_send.at[seq * OWNERS + k],
            decay_recv.at[slot], owner(seq, k),
        )

    def back(index, seq, k):
        return remote(
            starts.at[index], slice_of(incoming, seq, k), back_send.at[index],
            back_recv.at[seq * OWNERS + k], device(index),
        )

    rows = lax.broadcasted_iota(jnp.int32, (CHUNK, LANES), 0)
    columns = lax.broadcasted_iota(jnp.int32, (CHUNK, LANES), 1)

    def wide_row(index):
        return jnp.concatenate(
            [params_ref[index : index + 1, pl.ds(core_lane, inner)], params_ref[index : index + 1, model:]],
            axis=1,
        )

    def scan_chunk(seq, chunk):
        row0 = pl.multiple_of(chunk * CHUNK, CHUNK)
        window = pl.ds(row0, CHUNK + HALO)
        near_map = proj[seq, window, 0:LANES].astype(F32)
        other_map = far_map[seq, window, :].astype(F32)
        mixed = jnp.concatenate(
            [
                proj[seq, window, 2 * LANES :].astype(F32),
                jnp.where(core == 0, near_map, other_map),
                jnp.where(core == 0, other_map, near_map),
            ],
            axis=1,
        )
        conv = wide_row(4)
        for k in range(4):
            conv = conv + wide_row(k) * mixed[HALO - 3 + k : HALO - 3 + k + CHUNK]
        act = (conv * jax.nn.sigmoid(conv)).astype(BF16)
        value = act[:, :inner]
        in_map = act[:, inner : inner + LANES]
        out_map = act[:, inner + LANES :]

        raw = proj[seq, pl.ds(row0 + HALO, CHUNK), LANES : 2 * LANES].astype(F32)
        raw = raw + heads_ref[core, 0:1, :]
        tail = jnp.exp(-jnp.abs(raw))
        series = tail * (1.0 - tail * (0.5 - tail * (1.0 / 3.0 - 0.25 * tail)))
        step = jnp.maximum(raw, 0.0) + jnp.where(tail < 0.01, series, jnp.log(1.0 + tail))
        step = jnp.where((rows + row0).astype(F32) < live[seq, 0:1, :], step, 0.0)
        log_decay = -(step * heads_ref[core, 1:2, :]) * LOG2E
        cum = dot(tri_ref[...], jnp.concatenate(split3(log_decay), axis=0))
        shifted = jnp.where(step > 0.0, cum - jnp.log(step) * LOG2E, 1e30).T
        causal = rows >= columns
        scores = lax.dot_general(
            out_map, in_map, (((1,), (1,)), ((), ())), preferred_element_type=F32
        )
        before = state[seq]
        growth = dot(jnp.concatenate(split3(jnp.exp2(cum)), axis=1), spread_ref[...])
        reach = dot(
            jnp.concatenate([out_map, out_map], axis=1), jnp.concatenate(split2(before), axis=0)
        )
        base = growth * reach + params_ref[6:7, pl.ds(core_lane, inner)] * value.astype(F32)
        left = columns < LANES // 2
        zero = jnp.zeros((CHUNK, LANES), BF16)
        for tile in range(inner // LANES):
            lanes = slice(tile * LANES, (tile + 1) * LANES)
            result = base[:, lanes]
            for side in range(2):
                head = tile * 2 + side
                reached = jnp.where(
                    causal, cum[:, head : head + 1] - shifted[head : head + 1, :], -1e30
                )
                mixing = jnp.exp2(reached) * scores
                kept = jnp.where(left if side == 0 else ~left, value[:, lanes], zero)
                result = result + dot(
                    jnp.concatenate(split2(mixing), axis=1), jnp.concatenate([kept, kept], axis=0)
                )
            y_all[seq, pl.ds(row0, CHUNK), lanes] = result

        last = cum[CHUNK - 1 : CHUNK, :]
        to_end = jnp.exp2(last - cum) * step
        weighted = value.astype(F32) * dot(
            jnp.concatenate(split3(to_end), axis=1), spread_ref[...]
        )
        added = lax.dot_general(
            jnp.concatenate([in_map, in_map], axis=0),
            jnp.concatenate(split2(weighted), axis=0),
            (((0,), (0,)), ((), ())),
            preferred_element_type=F32,
        )
        state[seq] = growth[CHUNK - 1 : CHUNK, :] * before + added
        map_all[seq, pl.ds(row0, CHUNK), :] = out_map
        cum_all[seq, pl.ds(row0, CHUNK), :] = cum + total[seq]
        total[seq] = total[seq] + last

    state[...] = jnp.zeros_like(state)
    total[...] = jnp.zeros_like(total)
    ring_forward(1, 2)

    @pl.loop(0, 2)
    def _(seq):
        @pl.loop(0, slots // CHUNK)
        def _(chunk):
            scan_chunk(seq, chunk)

        @pl.loop(0, OWNERS)
        def _(i):
            k = lax.rem(my_k + i, OWNERS)
            mine = jnp.logical_and(i == 0, seq == my_seq)

            @pl.when(jnp.logical_not(mine))
            def _():
                decay_copy(seq, k, me).start()
                piece(seq, k, me).start()

            @pl.when(mine)
            def _():
                arrived[me] = slice_of(state, seq, k)[...]
                decays[me] = total[seq]

    def compose_all():
        @pl.loop(1, COUNT)
        def _(i):
            peer = lax.rem(me + i, COUNT)
            decay_copy(my_seq, my_k, peer).wait_recv()
            piece(my_seq, my_k, peer).wait_recv()

        column = pl.multiple_of(lax.rem(my_k, 2) * wide, LANES)
        decay = jnp.exp2(decays[...].reshape(COUNT, LANES))
        factors[...] = dot(
            jnp.concatenate(split3(decay), axis=1), spread_ref[:, pl.ds(column, wide)]
        )

        def compose(index, carry):
            starts[index] = carry
            return factors[pl.ds(index, 1), :] * carry + arrived[index]

        lax.fori_loop(0, COUNT, compose, jnp.zeros((8, wide), F32))

        @pl.loop(1, COUNT)
        def _(i):
            back(lax.rem(me + i, COUNT), my_seq, my_k).start()

        slice_of(incoming, my_seq, my_k)[...] = starts[me]

    pl.when(my_seq == 0)(compose_all)
    ring_finish(1)
    project(1, 0, 4)
    pl.when(my_seq == 1)(compose_all)
    project(1, 4, 10)

    def square_copy(seq):
        return remote(
            square.at[seq], far_square.at[seq], square_send.at[seq], square_recv.at[seq], partner
        )

    def gate_sequence(seq):
        @pl.loop(0, OWNERS)
        def _(k):
            @pl.when(jnp.logical_not(jnp.logical_and(k == my_k, my_seq == seq)))
            def _():
                back(me, seq, k).wait_recv()

        start = jnp.concatenate(split2(incoming[seq]), axis=0)

        @pl.loop(0, slots // CHUNK)
        def _(chunk):
            row0 = pl.multiple_of(chunk * CHUNK, CHUNK)
            here_rows = pl.ds(row0, CHUNK)
            growth = dot(
                jnp.concatenate(split3(jnp.exp2(cum_all[seq, here_rows, :])), axis=1),
                spread_ref[...],
            )
            out_map = map_all[seq, here_rows, :]
            reach = dot(jnp.concatenate([out_map, out_map], axis=1), start)
            gate = proj[seq, pl.ds(row0 + HALO, CHUNK), 0:inner].astype(F32)
            gated = (y_all[seq, here_rows, :] + growth * reach) * (gate * jax.nn.sigmoid(gate))
            y_all[seq, here_rows, :] = gated
            square[seq, here_rows, :] = jnp.broadcast_to(
                jnp.sum(gated * gated, axis=1, keepdims=True), (CHUNK, LANES)
            )

        square_copy(seq).start()

    for seq in range(2):
        gate_sequence(seq)

    out_copy = remote(staged, out_ref.at[:, pl.ds(core_lane, inner)], out_send, out_recv, partner)
    for seq in range(2):
        square_copy(seq).wait_recv()

        def normed(row0):
            here_rows = pl.ds(row0, CHUNK)
            mean = (square[seq, here_rows, 0:1] + far_square[seq, here_rows, 0:1]) / model
            result = (
                y_all[seq, here_rows, :]
                * lax.rsqrt(mean + 1e-05)
                * params_ref[5:6, pl.ds(core_lane, inner)]
            )
            kept = (rows[:, 0:1] + row0).astype(F32) < live[seq, 0:1, 0:1]
            return jnp.where(kept, result, 0.0).astype(BF16)

        @pl.when(core == seq)
        def _():
            @pl.loop(0, slots // CHUNK)
            def _(chunk):
                row0 = pl.multiple_of(chunk * CHUNK, CHUNK)
                out_ref[pl.ds(row0, CHUNK), pl.ds(core_lane, inner)] = normed(row0)

        @pl.when(core != seq)
        def _():
            @pl.loop(0, slots // CHUNK)
            def _(chunk):
                row0 = pl.multiple_of(chunk * CHUNK, CHUNK)
                staged[pl.ds(row0, CHUNK), :] = normed(row0)

            out_copy.start()

    for step in (1, 2, 3):
        part_copy(step).wait_send()
    live_copy.wait_send()

    @pl.when(me < COUNT - 1)
    def _():
        for side in range(2):
            edge_copy(side).wait_send()

    for group in range(2):
        for stage in range(3):
            for color in range(3):
                for slot in range(6):
                    ring_copy(group, color, stage, slot).wait_send()

    @pl.loop(0, 2 * OWNERS)
    def _(i):
        seq = i // OWNERS
        k = lax.rem(i, OWNERS)

        @pl.when(jnp.logical_not(jnp.logical_and(k == my_k, my_seq == seq)))
        def _():
            piece(seq, k, me).wait_send()
            decay_copy(seq, k, me).wait_send()

    @pl.loop(1, COUNT)
    def _(i):
        back(lax.rem(me + i, COUNT), my_seq, my_k).wait_send()

    for seq in range(2):
        square_copy(seq).wait_send()
    out_copy.wait_send()
    far_lane = pl.multiple_of((1 - core) * inner, LANES)
    remote(
        staged, out_ref.at[:, pl.ds(far_lane, inner)], out_send, out_recv, partner
    ).wait_recv()


def layer_call(live, edge, tokens, pieces, params, heads, spread, tri):
    slots, model = tokens.shape
    inner = model // 2
    columns = pieces.shape[2]
    padded = slots + HALO
    vmem = pl.BlockSpec(memory_space=pltpu.VMEM)
    dma = pltpu.SemaphoreType.DMA
    return pl.pallas_call(
        layer_kernel,
        out_shape=jax.ShapeDtypeStruct((slots, model), BF16),
        in_specs=[vmem, vmem, pl.BlockSpec(memory_space=pl.ANY)] + [vmem] * 5,
        out_specs=vmem,
        scratch_shapes=[
            pltpu.VMEM((2, padded, model), BF16),
            pltpu.VMEM((2, 2, 4, 4, 2, model // 32, columns // 2), BF16),
            pltpu.VMEM((2, padded, columns), BF16),
            pltpu.VMEM((2, padded, LANES), BF16),
            pltpu.VMEM((2, slots, inner), F32),
            pltpu.VMEM((2, slots, LANES), BF16),
            pltpu.VMEM((2, slots, LANES), F32),
            pltpu.VMEM((2, LANES, inner), F32),
            pltpu.VMEM((2, 1, LANES), F32),
            pltpu.VMEM(pieces.shape, BF16),
            pltpu.VMEM((model // 32, columns), BF16),
            pltpu.VMEM((COUNT, 8, inner // 2), F32),
            pltpu.VMEM((COUNT, 8, inner // 2), F32),
            pltpu.VMEM((COUNT, 1, LANES), F32),
            pltpu.VMEM((COUNT, inner // 2), F32),
            pltpu.VMEM((2, LANES, inner), F32),
            pltpu.VMEM((2, slots, LANES), F32),
            pltpu.VMEM((2, slots, LANES), F32),
            pltpu.VMEM((slots, inner), BF16),
            pltpu.VMEM((2, 8, LANES), F32),
            dma((4,)), dma((4,)),
            dma, dma, dma,
            dma((2,)), dma((2,)),
            dma, dma,
            dma((2, 3, 3, 6)), dma((2, 3, 3, 6)),
            dma, dma,
            dma((COUNT,)), dma((COUNT,)), dma((COUNT,)), dma((COUNT,)),
            dma((COUNT,)), dma((COUNT,)),
            dma((2,)), dma((2,)),
            dma, dma,
        ],
        compiler_params=pltpu.CompilerParams(
            collective_id=0, has_side_effects=True, vmem_limit_bytes=67043328
        ),
        name="layer",
    )(live, edge, tokens, pieces, params, heads, spread, tri)


def local(
    tokens, bounds, in_weight, conv_weight, conv_bias, dt_bias, decay_rate, skip_gain, norm_gain
):
    slots, model = tokens.shape[1:]
    width = norm_gain.shape[0]
    inner = width // 2
    heads = decay_rate.shape[0] // 2
    rows = in_weight.shape[0]

    low, high = 4 * LANES, 6 * LANES
    pieces = []
    for side in range(2):
        for core in range(2):
            value = width + core * inner
            gate = core * inner
            if side == 0:
                raw = 2 * width + 2 * LANES + core * heads
                pieces += [
                    in_weight[:, 2 * width + core * LANES : 2 * width + (core + 1) * LANES],
                    jnp.pad(in_weight[:, raw : raw + heads], ((0, 0), (0, LANES - heads))),
                    in_weight[:, value : value + low],
                    in_weight[:, gate : gate + high],
                ]
            else:
                pieces += [
                    in_weight[:, value + low : value + inner],
                    in_weight[:, gate + high : gate + inner],
                    jnp.zeros((rows, 2 * high - inner), BF16),
                ]
    pieces = jnp.concatenate(pieces, axis=1).reshape(rows, 4, 2 * high).swapaxes(0, 1)

    blocks = bounds[0, 0, 1] - bounds[0, 0, 0]
    edge = lax.dynamic_slice_in_dim(tokens[0], blocks * BLOCK - HALO, HALO, 0)
    live = jnp.full((8, LANES), (blocks * BLOCK).astype(F32))
    stretch = lambda a: jnp.pad(a, (0, conv_bias.shape[0] - width))[None]
    params = jnp.concatenate(
        [
            conv_weight, conv_bias[None], stretch(norm_gain),
            stretch(jnp.repeat(skip_gain, width // (2 * heads))),
            jnp.zeros((1, conv_bias.shape[0]), F32),
        ]
    )
    per_head = jnp.stack([dt_bias.reshape(2, heads), decay_rate.reshape(2, heads)], axis=1)
    per_head = jnp.pad(per_head, ((0, 0), (0, 6), (0, LANES - heads)))
    spread = (np.arange(inner)[None, :] // (inner // heads) == np.arange(LANES)[:, None])
    spread = jnp.asarray(np.concatenate([spread] * 3, axis=0), BF16)
    tri = jnp.asarray(np.concatenate([np.tril(np.ones((CHUNK, CHUNK)))] * 3, axis=1), BF16)
    out = layer_call(live, edge, tokens[0], pieces, params, per_head, spread, tri)
    return out[None]


def solution(mesh):
    split = Mesh(mesh.devices.reshape(4, 4, 2, 2, 2), AXES + ("core",))
    return jax.shard_map(
        local,
        mesh=split,
        in_specs=(
            P("core", AXES, None),
            P("core", AXES, None),
            P(AXES + ("core",), None),
            P(), P(), P(), P(), P(), P(),
        ),
        out_specs=P("core", AXES, None),
        check_vma=False,
    )
```

```python
import jax
import jax.numpy as jnp
from jax import lax
from jax.experimental import pallas as pl
from jax.experimental.pallas import tpu as pltpu
from jax.sharding import Mesh
from jax.sharding import PartitionSpec as P

BLOCK = 256
CHUNK = 128
HALO = 16
LANES = 128
COUNT = 64
OWNERS = 32
LOG2E = 1.4426950408889634
AXES = ("y", "z", "xh", "xl")
F32 = jnp.float32
BF16 = jnp.bfloat16
MESH = pl.DeviceIdType.MESH
ORDERS = (("x", "y", "z"), ("y", "z", "x"), ("z", "x", "y"))
GROUPS = (
    (((0, 128), (128, 128), (256, 128)), 48),
    (((384, 128), (512, 128), (640, 128)), 32),
    (((768, 256), (1024, 256), (1280, 128)), 48),
)
SLOTS = ((0, 0, 1), (0, 1, 1), (-1, 0, 1), (0, 1, -1), (0, 0, -1), (1, 1, -1))


def split3(value):
    hi = value.astype(BF16)
    rest = value - hi.astype(F32)
    mid = rest.astype(BF16)
    lo = (rest - mid.astype(F32)).astype(BF16)
    return hi, mid, lo


def split2(value):
    hi = value.astype(BF16)
    lo = (value - hi.astype(F32)).astype(BF16)
    return hi, lo


def dot(a, b):
    return jnp.dot(a, b, preferred_element_type=F32)


def layer_kernel(
    bounds_ref, tokens_ref, shard_ref, taps_ref, bias_ref, dt_ref, decay_ref, skip_ref, gain_ref,
    out_ref,
    rows_in, weight, act_all, raw_all, spread_ref, tri_ref, heads, skips, pieces, ends, edge,
    far_map, y_all, map_all, cum_all, state, total, parts, block, arrived,
    starts, decays, factors, incoming, square, far_square, staged, live,
    end_sem, part_send, part_recv, token_sem, token_send, token_recv, edge_send, edge_recv, live_send,
    live_recv, gather_send, gather_recv, map_send, map_recv, piece_send, piece_recv, decay_send,
    decay_recv, back_send, back_recv, square_send, square_recv, out_send, out_recv,
):
    y, z, xh, xl = (lax.axis_index(axis) for axis in AXES)
    core = lax.axis_index("core")
    x = xh * 2 + xl
    here = {"y": y, "z": z, "x": x}
    me = (y * 4 + z) * 4 + x
    slots, model = tokens_ref.shape[1:]
    inner = model // 2
    wide = inner // 2
    head_count = dt_ref.shape[1] // 2
    shard = tokens_ref.at[0]
    partner = {"core": 1 - core}
    core_lane = pl.multiple_of(core * inner, LANES)

    def device(index):
        return {
            "y": index // 16,
            "z": lax.rem(index // 4, 4),
            "xh": lax.rem(index // 2, 2),
            "xl": lax.rem(index, 2),
        }

    def remote(source, target, send, recv, where):
        return pltpu.make_async_remote_copy(
            src_ref=source, dst_ref=target, send_sem=send, recv_sem=recv,
            device_id=where, device_id_type=MESH,
        )

    barrier = pltpu.get_barrier_semaphore()

    @pl.loop(1, 2 * COUNT)
    def _(i):
        other = lax.rem(me * 2 + core + i, 2 * COUNT)
        pl.semaphore_signal(
            barrier, inc=1, device_id={**device(other // 2), "core": lax.rem(other, 2)},
            device_id_type=MESH,
        )

    own_rows = pltpu.make_async_copy(shard, rows_in.at[core, pl.ds(HALO, slots)], token_sem)
    own_rows.start()
    end_copies = [
        pltpu.make_async_copy(
            shard.at[pl.ds((i + 1) * BLOCK - HALO, HALO)], ends.at[i], end_sem.at[i]
        )
        for i in range(slots // BLOCK)
    ]
    for copy in end_copies:
        copy.start()

    t = LANES
    for side in range(2):
        for other in range(2):
            index = side * 2 + other
            value, gate = model + other * inner, other * inner
            if side == 0:
                maps = 2 * model + other * t
                raw = 2 * model + 2 * t
                pieces[index, :, 0:t] = shard_ref[:, maps : maps + t]
                pieces[index, :, t : 2 * t] = jnp.zeros((shard_ref.shape[0], t), BF16)
                pieces[index, :, t : t + 2 * head_count] = shard_ref[:, raw : raw + 2 * head_count]
                pieces[index, :, 2 * t : 3 * t] = shard_ref[:, value : value + t]
                pieces[index, :, 3 * t : 6 * t] = shard_ref[:, value + 4 * t : value + 7 * t]
                pieces[index, :, 6 * t :] = shard_ref[:, gate : gate + 5 * t]
            else:
                pieces[index, :, 0 : 3 * t] = shard_ref[:, value + t : value + 4 * t]
                pieces[index, :, 3 * t : 6 * t] = shard_ref[:, value + 7 * t : value + 10 * t]
                pieces[index, :, 6 * t :] = shard_ref[:, gate + 5 * t : gate + 10 * t]

    block_count = bounds_ref[0, 0, 1] - bounds_ref[0, 0, 0]
    live[core] = jnp.full((8, LANES), (block_count * BLOCK).astype(F32))
    heads[...] = jnp.zeros_like(heads)
    for i, ref in enumerate((dt_ref, decay_ref, skip_ref)):
        heads[i : i + 1, 0 : 2 * head_count] = ref[...]
    both = heads[...]
    mine = jnp.where(core == 0, both, pltpu.roll(both, LANES - head_count, 1))
    lane8 = lax.broadcasted_iota(jnp.int32, (8, LANES), 1)
    heads[...] = jnp.where(lane8 < head_count, mine, 0.0)
    pl.semaphore_wait(barrier, 2 * COUNT - 1)

    my_part = xl * 2 + core

    def part_copy(step):
        target = lax.rem(my_part + step, 4)
        return remote(
            pieces.at[target], parts.at[my_part], part_send.at[step], part_recv.at[step],
            {"xl": target // 2, "core": lax.rem(target, 2)},
        )

    def part_arrival(step):
        source = lax.rem(my_part + 4 - step, 4)
        return remote(
            pieces.at[0], parts.at[source], part_send.at[step], part_recv.at[step], partner
        )

    for step in (1, 2, 3):
        part_copy(step).start()
    parts[my_part] = pieces[my_part]

    rows_copy = remote(
        shard, rows_in.at[core, pl.ds(HALO, slots)], token_send, token_recv, partner
    )
    live_copy = remote(live.at[core], live.at[core], live_send, live_recv, partner)
    live_copy.start()
    for copy in end_copies:
        copy.wait()
    chosen = ends[0].astype(F32)
    for i in range(1, slots // BLOCK):
        chosen = jnp.where(block_count == i + 1, ends[i].astype(F32), chosen)
    edge[...] = chosen.astype(BF16)

    def edge_copy(side):
        return remote(
            edge, rows_in.at[core, pl.ds(0, HALO)], edge_send.at[side], edge_recv.at[core],
            {**device(me + 1), "core": side},
        )

    @pl.when(me < COUNT - 1)
    def _():
        for side in range(2):
            edge_copy(side).start()

    @pl.when(me == 0)
    def _():
        rows_in[:, 0:HALO, :] = jnp.zeros((2, HALO, model), BF16)

    for step in (1, 2, 3):
        part_arrival(step).wait_recv()
    block[...] = jnp.concatenate([parts[i].astype(F32) for i in range(4)], axis=0).astype(BF16)

    near = lambda axis, step: lax.rem(here[axis] + step + 4, 4)

    def along(axis, step):
        coordinate = near(axis, step)
        if axis == "x":
            return {"xh": coordinate // 2, "xl": lax.rem(coordinate, 2)}
        return {axis: coordinate}

    def part_of(group, color, half):
        start, size = GROUPS[group][0][color]
        cut = GROUPS[group][1]
        rows = pl.ds(0, cut) if half == 0 else pl.ds(cut, block.shape[0] - cut)
        return rows, pl.ds(start, size)

    def region(group, color, half, spot):
        wy, wz, wx = (spot[axis] for axis in ("y", "z", "x"))
        low, high = (slice(None), slice(None)) if wx is None else (lax.rem(wx, 2), wx // 2)
        wy = slice(None) if wy is None else wy
        wz = slice(None) if wz is None else wz
        return weight.at[(low, wy, wz, high) + part_of(group, color, half)]

    def spot_of(color, stage, coordinate):
        spot = dict(here)
        for axis in ORDERS[color][:stage]:
            spot[axis] = None
        spot[ORDERS[color][stage]] = coordinate
        return spot

    def ring_copy(group, color, stage, slot):
        offset, half, step = SLOTS[slot]
        axis = ORDERS[color][stage]
        target = region(group, color, half, spot_of(color, stage, near(axis, offset)))
        source = target
        if stage == 0 and offset == 0:
            source = block.at[part_of(group, color, half)]
        return remote(
            source, target, gather_send.at[group, color, stage, slot],
            gather_recv.at[group, color, stage, slot], along(axis, step),
        )

    def ring_arrival(group, color, stage, slot):
        offset, half, step = SLOTS[slot]
        axis = ORDERS[color][stage]
        target = region(group, color, half, spot_of(color, stage, near(axis, offset - step)))
        return remote(
            target, target, gather_send.at[group, color, stage, slot],
            gather_recv.at[group, color, stage, slot], along(axis, step),
        )

    def ring_start(group, stage):
        for color in range(3):
            if stage:
                for slot in (1, 2, 4, 5):
                    ring_arrival(group, color, stage - 1, slot).wait_recv()
            for slot in (0, 3, 1, 4):
                ring_copy(group, color, stage, slot).start()

    def ring_forward(group, stage):
        for color in range(3):
            ring_arrival(group, color, stage, 0).wait_recv()
            ring_copy(group, color, stage, 2).start()
            ring_arrival(group, color, stage, 3).wait_recv()
            ring_copy(group, color, stage, 5).start()

    def ring_finish(group):
        for color in range(3):
            for slot in (1, 2, 4, 5):
                ring_arrival(group, color, 2, slot).wait_recv()

    ring_start(0, 0)
    rows_copy.start()
    weight[xl, y, z, xh] = block[...]
    ring_forward(0, 0)
    ring_start(0, 1)
    ring_start(1, 0)
    lane = lax.broadcasted_iota(jnp.int32, (LANES, inner), 1)
    first = lax.broadcasted_iota(jnp.int32, (LANES, inner), 0) * (inner // head_count)
    ones = jnp.where(
        jnp.logical_and(lane >= first, lane < first + inner // head_count), 1.0, 0.0
    ).astype(BF16)
    rows = lax.broadcasted_iota(jnp.int32, (CHUNK, LANES), 0)
    columns = lax.broadcasted_iota(jnp.int32, (CHUNK, LANES), 1)
    below = jnp.where(rows >= columns, 1.0, 0.0).astype(BF16)
    for i in range(3):
        spread_ref[i * LANES : (i + 1) * LANES, :] = ones
        tri_ref[:, i * LANES : (i + 1) * LANES] = below
    ring_forward(0, 1)
    ring_forward(1, 0)
    ring_start(0, 2)
    ring_start(1, 1)
    skips[...] = dot(jnp.concatenate(split3(heads[...]), axis=1), spread_ref[...])
    ring_forward(0, 2)
    ring_forward(1, 1)
    ring_start(1, 2)
    ring_start(2, 0)
    own_rows.wait()
    rows_copy.wait_send()
    remote(
        shard, rows_in.at[1 - core, pl.ds(HALO, slots)], token_send, token_recv, partner
    ).wait_recv()
    remote(live.at[core], live.at[1 - core], live_send, live_recv, partner).wait_recv()

    @pl.when(me > 0)
    def _():
        for side in range(2):
            remote(
                edge, rows_in.at[side, pl.ds(0, HALO)], edge_send.at[side], edge_recv.at[side],
                partner,
            ).wait_recv()

    ring_finish(0)

    def matrix(start):
        picked = pl.ds(pl.multiple_of(start, LANES), LANES)
        pair = [weight[i, :, :, :, :, picked].reshape(model, LANES) for i in range(2)]
        return jnp.concatenate(pair, axis=1)

    def both_lanes(ref, row, starts):
        return jnp.concatenate([ref[row : row + 1, pl.ds(start, LANES)] for start in starts], axis=1)

    def project_mixed(group, seq, color):
        result = dot(rows_in[seq], matrix(GROUPS[group][0][0][0] + color * LANES)).astype(BF16)
        tiles = [group * 6 + color, group * 6 + color + 3]
        if group == 0:
            raw_all[seq, jnp.where(color == 1, 1, 0)] = result[HALO:, 0:LANES]
        lanes = [
            pl.multiple_of(
                jnp.where(
                    tile == 0, model + core * LANES, core * inner + jnp.maximum(tile - 2, 0) * LANES
                ),
                LANES,
            )
            for tile in tiles
        ]
        mixed = result.astype(F32)
        conv = both_lanes(bias_ref, 0, lanes)
        for k in range(4):
            conv = conv + both_lanes(taps_ref, k, lanes) * mixed[HALO - 3 + k : HALO - 3 + k + slots]
        act = (conv * jax.nn.sigmoid(conv)).astype(BF16)
        for i, tile in enumerate(tiles):
            act_all[seq, :, pl.ds(pl.multiple_of(tile * LANES, LANES), LANES)] = act[
                :, i * LANES : (i + 1) * LANES
            ]

    def project_gate(first, last):
        @pl.loop(first, last)
        def _(i):
            seq = i // 5
            color = lax.rem(i, 5)
            result = dot(rows_in[seq, HALO:, :], matrix(GROUPS[2][0][0][0] + color * LANES))
            for half in range(2):
                tile = pl.ds(pl.multiple_of((half * 5 + color) * LANES, LANES), LANES)
                act_all[seq, :, tile] = result[:, half * LANES : (half + 1) * LANES].astype(BF16)

    map_copy = remote(act_all.at[:, :, pl.ds(0, LANES)], far_map, map_send, map_recv, partner)

    @pl.loop(0, 6)
    def _(i):
        project_mixed(0, lax.rem(i, 2), i // 2)

        @pl.when(i == 2)
        def _():
            ring_forward(1, 2)
            ring_forward(2, 0)
            ring_start(2, 1)

        @pl.when(i == 3)
        def _():
            map_copy.start()

    ring_finish(1)

    def slice_of(ref, seq, k):
        row = pl.multiple_of(k // 2 * 8, 8)
        column = pl.multiple_of(lax.rem(k, 2) * wide, LANES)
        return ref.at[seq, pl.ds(row, 8), pl.ds(column, wide)]

    my_k = (y * 4 + z) * 2 + xh
    my_seq = lax.rem(y + z + xl, 2)

    def owner(seq, k):
        oy, oz = k // 8, lax.rem(k // 2, 4)
        return {"y": oy, "z": oz, "xh": lax.rem(k, 2), "xl": lax.rem(seq + oy + oz, 2)}

    def piece(seq, k, slot):
        return remote(
            slice_of(state, seq, k), arrived.at[slot], piece_send.at[seq * OWNERS + k],
            piece_recv.at[slot], owner(seq, k),
        )

    def decay_copy(seq, k, slot):
        return remote(
            total.at[seq], decays.at[slot], decay_send.at[seq * OWNERS + k],
            decay_recv.at[slot], owner(seq, k),
        )

    def back(index, seq, k):
        return remote(
            starts.at[index], slice_of(incoming, seq, k), back_send.at[index],
            back_recv.at[seq * OWNERS + k], device(index),
        )

    def scan_chunk(seq, chunk):
        row0 = pl.multiple_of(chunk * CHUNK, CHUNK)
        window = pl.ds(row0, CHUNK)
        near_map = act_all[seq, window, 0:LANES]
        other_map = far_map[seq, window, :]
        in_map = jnp.where(core == 0, near_map, other_map)
        out_map = jnp.where(core == 0, other_map, near_map)
        value = act_all[seq, window, 2 * LANES :]

        raw = raw_all[seq, 1, window, :].astype(F32)
        raw = jnp.where(core == 0, raw, pltpu.roll(raw, LANES - head_count, 1))
        raw = raw + heads[0:1, :]
        tail = jnp.exp(-jnp.abs(raw))
        series = tail * (1.0 - tail * (0.5 - tail * (1.0 / 3.0 - 0.25 * tail)))
        step = jnp.maximum(raw, 0.0) + jnp.where(tail < 0.01, series, jnp.log(1.0 + tail))
        step = jnp.where((rows + row0).astype(F32) < live[seq, 0:1, :], step, 0.0)
        log_decay = -(step * heads[1:2, :]) * LOG2E
        cum = dot(tri_ref[...], jnp.concatenate(split3(log_decay), axis=0))
        shifted = jnp.where(step > 0.0, cum - jnp.log(step) * LOG2E, 1e30).T
        causal = rows >= columns
        scores = lax.dot_general(
            out_map, in_map, (((1,), (1,)), ((), ())), preferred_element_type=F32
        )
        before = state[seq]
        growth = dot(jnp.concatenate(split3(jnp.exp2(cum)), axis=1), spread_ref[...])
        reach = dot(
            jnp.concatenate([out_map, out_map], axis=1), jnp.concatenate(split2(before), axis=0)
        )
        base = growth * reach + skips[2:3, :] * value.astype(F32)
        left = columns < LANES // 2
        zero = jnp.zeros((CHUNK, LANES), BF16)
        for tile in range(inner // LANES):
            lanes = slice(tile * LANES, (tile + 1) * LANES)
            result = base[:, lanes]
            for side in range(2):
                head = tile * 2 + side
                reached = jnp.where(
                    causal, cum[:, head : head + 1] - shifted[head : head + 1, :], -1e30
                )
                mixing = jnp.exp2(reached) * scores
                kept = jnp.where(left if side == 0 else ~left, value[:, lanes], zero)
                result = result + dot(
                    jnp.concatenate(split2(mixing), axis=1), jnp.concatenate([kept, kept], axis=0)
                )
            y_all[seq, pl.ds(row0, CHUNK), lanes] = result

        last = cum[CHUNK - 1 : CHUNK, :]
        to_end = jnp.exp2(last - cum) * step
        weighted = value.astype(F32) * dot(
            jnp.concatenate(split3(to_end), axis=1), spread_ref[...]
        )
        added = lax.dot_general(
            jnp.concatenate([in_map, in_map], axis=0),
            jnp.concatenate(split2(weighted), axis=0),
            (((0,), (0,)), ((), ())),
            preferred_element_type=F32,
        )
        state[seq] = growth[CHUNK - 1 : CHUNK, :] * before + added
        map_all[seq, pl.ds(row0, CHUNK), :] = out_map
        cum_all[seq, pl.ds(row0, CHUNK), :] = cum + total[seq]
        total[seq] = total[seq] + last

    def compose_all():
        @pl.loop(1, COUNT)
        def _(i):
            peer = lax.rem(me + i, COUNT)
            decay_copy(my_seq, my_k, peer).wait_recv()
            piece(my_seq, my_k, peer).wait_recv()

        column = pl.multiple_of(lax.rem(my_k, 2) * wide, LANES)
        decay = jnp.exp2(decays[...].reshape(COUNT, LANES))
        factors[...] = dot(
            jnp.concatenate(split3(decay), axis=1), spread_ref[:, pl.ds(column, wide)]
        )

        def compose(index, carry):
            starts[index] = carry
            return factors[pl.ds(index, 1), :] * carry + arrived[index]

        lax.fori_loop(0, COUNT, compose, jnp.zeros((8, wide), F32))

        @pl.loop(1, COUNT)
        def _(i):
            back(lax.rem(me + i, COUNT), my_seq, my_k).start()

        slice_of(incoming, my_seq, my_k)[...] = starts[me]

    state[...] = jnp.zeros_like(state)
    total[...] = jnp.zeros_like(total)

    @pl.loop(0, 2)
    def _(seq):
        @pl.loop(0, 3)
        def _(color):
            project_mixed(1, seq, color)

        @pl.when(seq == 0)
        def _():
            ring_forward(2, 1)
            ring_start(2, 2)
            map_copy.wait()

        @pl.loop(0, slots // CHUNK)
        def _(chunk):
            scan_chunk(seq, chunk)

            @pl.when(jnp.logical_and(jnp.logical_and(seq == 1, chunk == 3), my_seq == 0))
            def _():
                compose_all()

        @pl.when(seq == 0)
        def _():
            ring_forward(2, 2)

        @pl.loop(0, OWNERS)
        def _(i):
            k = lax.rem(my_k + i, OWNERS)
            mine = jnp.logical_and(i == 0, seq == my_seq)

            @pl.when(jnp.logical_not(mine))
            def _():
                decay_copy(seq, k, me).start()
                piece(seq, k, me).start()

            @pl.when(mine)
            def _():
                arrived[me] = slice_of(state, seq, k)[...]
                decays[me] = total[seq]

    ring_finish(2)
    project_gate(0, 8)
    pl.when(my_seq == 1)(compose_all)
    project_gate(8, 10)

    def square_copy(seq):
        return remote(
            square.at[seq], far_square.at[seq], square_send.at[seq], square_recv.at[seq], partner
        )

    def gate_sequence(seq):
        @pl.loop(0, OWNERS)
        def _(k):
            @pl.when(jnp.logical_not(jnp.logical_and(k == my_k, my_seq == seq)))
            def _():
                back(me, seq, k).wait_recv()

        start = jnp.concatenate(split2(incoming[seq]), axis=0)

        @pl.loop(0, slots // CHUNK)
        def _(chunk):
            row0 = pl.multiple_of(chunk * CHUNK, CHUNK)
            here_rows = pl.ds(row0, CHUNK)
            growth = dot(
                jnp.concatenate(split3(jnp.exp2(cum_all[seq, here_rows, :])), axis=1),
                spread_ref[...],
            )
            out_map = map_all[seq, here_rows, :]
            reach = dot(jnp.concatenate([out_map, out_map], axis=1), start)
            gate = act_all[seq, here_rows, 0:inner].astype(F32)
            gated = (y_all[seq, here_rows, :] + growth * reach) * (gate * jax.nn.sigmoid(gate))
            y_all[seq, here_rows, :] = gated
            square[seq, here_rows, :] = jnp.broadcast_to(
                jnp.sum(gated * gated, axis=1, keepdims=True), (CHUNK, LANES)
            )

        square_copy(seq).start()

    for seq in range(2):
        gate_sequence(seq)

    out_copy = remote(staged, out_ref.at[:, pl.ds(core_lane, inner)], out_send, out_recv, partner)
    for seq in range(2):
        square_copy(seq).wait_recv()

        def normed(row0):
            here_rows = pl.ds(row0, CHUNK)
            mean = (square[seq, here_rows, 0:1] + far_square[seq, here_rows, 0:1]) / model
            result = (
                y_all[seq, here_rows, :]
                * lax.rsqrt(mean + 1e-05)
                * gain_ref[0:1, pl.ds(core_lane, inner)]
            )
            kept = (rows[:, 0:1] + row0).astype(F32) < live[seq, 0:1, 0:1]
            return jnp.where(kept, result, 0.0).astype(BF16)

        @pl.when(core == seq)
        def _():
            @pl.loop(0, slots // CHUNK)
            def _(chunk):
                row0 = pl.multiple_of(chunk * CHUNK, CHUNK)
                out_ref[pl.ds(row0, CHUNK), pl.ds(core_lane, inner)] = normed(row0)

        @pl.when(core != seq)
        def _():
            @pl.loop(0, slots // CHUNK)
            def _(chunk):
                row0 = pl.multiple_of(chunk * CHUNK, CHUNK)
                staged[pl.ds(row0, CHUNK), :] = normed(row0)

            out_copy.start()

    for step in (1, 2, 3):
        part_copy(step).wait_send()
    live_copy.wait_send()

    @pl.when(me < COUNT - 1)
    def _():
        for side in range(2):
            edge_copy(side).wait_send()

    for group in range(3):
        for stage in range(3):
            for color in range(3):
                for slot in range(6):
                    ring_copy(group, color, stage, slot).wait_send()

    @pl.loop(0, 2 * OWNERS)
    def _(i):
        seq = i // OWNERS
        k = lax.rem(i, OWNERS)

        @pl.when(jnp.logical_not(jnp.logical_and(k == my_k, my_seq == seq)))
        def _():
            piece(seq, k, me).wait_send()
            decay_copy(seq, k, me).wait_send()

    @pl.loop(1, COUNT)
    def _(i):
        back(lax.rem(me + i, COUNT), my_seq, my_k).wait_send()

    for seq in range(2):
        square_copy(seq).wait_send()
    out_copy.wait_send()
    far_lane = pl.multiple_of((1 - core) * inner, LANES)
    remote(
        staged, out_ref.at[:, pl.ds(far_lane, inner)], out_send, out_recv, partner
    ).wait_recv()


def local(
    tokens, bounds, in_weight, conv_weight, conv_bias, dt_bias, decay_rate, skip_gain, norm_gain
):
    slots, model = tokens.shape[1:]
    inner = model // 2
    rows = in_weight.shape[0]
    padded = slots + HALO
    columns = 11 * LANES
    vmem = pl.BlockSpec(memory_space=pltpu.VMEM)
    dma = pltpu.SemaphoreType.DMA
    out = pl.pallas_call(
        layer_kernel,
        out_shape=jax.ShapeDtypeStruct((slots, model), BF16),
        in_specs=[
            pl.BlockSpec(memory_space=pltpu.SMEM), pl.BlockSpec(memory_space=pl.ANY),
        ] + [vmem] * 7,
        out_specs=vmem,
        scratch_shapes=[
            pltpu.VMEM((2, padded, model), BF16),
            pltpu.VMEM((2, 4, 4, 2, 4 * rows, columns), BF16),
            pltpu.VMEM((2, slots, 12 * LANES), BF16),
            pltpu.VMEM((2, 2, slots, LANES), BF16),
            pltpu.VMEM((3 * LANES, inner), BF16),
            pltpu.VMEM((CHUNK, 3 * LANES), BF16),
            pltpu.VMEM((8, LANES), F32),
            pltpu.VMEM((8, inner), F32),
            pltpu.VMEM((4, rows, columns), BF16),
            pltpu.VMEM((slots // BLOCK, HALO, model), BF16),
            pltpu.VMEM((HALO, model), BF16),
            pltpu.VMEM((2, slots, LANES), BF16),
            pltpu.VMEM((2, slots, inner), F32),
            pltpu.VMEM((2, slots, LANES), BF16),
            pltpu.VMEM((2, slots, LANES), F32),
            pltpu.VMEM((2, LANES, inner), F32),
            pltpu.VMEM((2, 1, LANES), F32),
            pltpu.VMEM((4, rows, columns), BF16),
            pltpu.VMEM((4 * rows, columns), BF16),
            pltpu.VMEM((COUNT, 8, inner // 2), F32),
            pltpu.VMEM((COUNT, 8, inner // 2), F32),
            pltpu.VMEM((COUNT, 1, LANES), F32),
            pltpu.VMEM((COUNT, inner // 2), F32),
            pltpu.VMEM((2, LANES, inner), F32),
            pltpu.VMEM((2, slots, LANES), F32),
            pltpu.VMEM((2, slots, LANES), F32),
            pltpu.VMEM((slots, inner), BF16),
            pltpu.VMEM((2, 8, LANES), F32),
            dma((slots // BLOCK,)),
            dma((4,)), dma((4,)),
            dma, dma, dma,
            dma((2,)), dma((2,)),
            dma, dma,
            dma((3, 3, 3, 6)), dma((3, 3, 3, 6)),
            dma, dma,
            dma((COUNT,)), dma((COUNT,)), dma((COUNT,)), dma((COUNT,)),
            dma((COUNT,)), dma((COUNT,)),
            dma((2,)), dma((2,)),
            dma, dma,
        ],
        compiler_params=pltpu.CompilerParams(
            collective_id=0, has_side_effects=True, vmem_limit_bytes=67043328
        ),
        name="layer",
    )(
        bounds, tokens, in_weight, conv_weight, conv_bias[None], dt_bias[None], decay_rate[None],
        skip_gain[None], norm_gain[None],
    )
    return out[None]


def solution(mesh):
    split = Mesh(mesh.devices.reshape(4, 4, 2, 2, 2), AXES + ("core",))
    return jax.shard_map(
        local,
        mesh=split,
        in_specs=(
            P("core", AXES, None),
            P("core", AXES, None),
            P(AXES + ("core",), None),
            P(), P(), P(), P(), P(), P(),
        ),
        out_specs=P("core", AXES, None),
        check_vma=False,
    )
```

```python
import jax
import jax.numpy as jnp
from jax import lax
from jax.experimental import pallas as pl
from jax.experimental.pallas import tpu as pltpu
from jax.sharding import Mesh
from jax.sharding import PartitionSpec as P

BLOCK = 256
CHUNK = 128
HALO = 16
LANES = 128
COUNT = 64
OWNERS = 32
LOG2E = 1.4426950408889634
AXES = ("y", "z", "xh", "xl")
F32 = jnp.float32
BF16 = jnp.bfloat16
MESH = pl.DeviceIdType.MESH
ORDERS = (("x", "y", "z"), ("y", "z", "x"), ("z", "x", "y"))
CUT = 48
GROUPS = (
    ((0, 1), (1, 1), (2, 1)),
    ((3, 1), (4, 1), (5, 1)),
    ((6, 2), (8, 2), (10, 1)),
)
SLOTS = ((0, 0, 1), (0, 1, 1), (-1, 0, 1), (0, 1, -1), (0, 0, -1), (1, 1, -1))


def split3(value):
    hi = value.astype(BF16)
    rest = value - hi.astype(F32)
    mid = rest.astype(BF16)
    lo = (rest - mid.astype(F32)).astype(BF16)
    return hi, mid, lo


def split2(value):
    hi = value.astype(BF16)
    lo = (value - hi.astype(F32)).astype(BF16)
    return hi, lo


def dot(a, b):
    return jnp.dot(a, b, preferred_element_type=F32)


def layer_kernel(
    bounds_ref, tokens_ref, shard_ref, taps_ref, bias_ref, dt_ref, decay_ref, skip_ref, gain_ref,
    out_ref,
    rows_in, top, bottom, act_all, raw_all, spread_ref, tri_ref, heads, skips, pieces, ends, edge,
    far_map, y_all, map_all, cum_all, state, total, parts, arrived,
    starts, decays, factors, incoming, square, far_square, staged, live, lift,
    end_sem, part_send, part_recv, token_sem, token_send, token_recv, edge_send, edge_recv, live_send,
    live_recv, gather_send, gather_recv, map_send, map_recv, piece_send, piece_recv, decay_send,
    decay_recv, back_send, back_recv, square_send, square_recv, out_send, out_recv,
):
    y, z, xh, xl = (lax.axis_index(axis) for axis in AXES)
    core = lax.axis_index("core")
    x = xh * 2 + xl
    here = {"y": y, "z": z, "x": x}
    me = (y * 4 + z) * 4 + x
    slots, model = tokens_ref.shape[1:]
    inner = model // 2
    wide = inner // 2
    head_count = dt_ref.shape[1] // 2
    shard = tokens_ref.at[0]
    partner = {"core": 1 - core}
    core_lane = pl.multiple_of(core * inner, LANES)

    def device(index):
        return {
            "y": index // 16,
            "z": lax.rem(index // 4, 4),
            "xh": lax.rem(index // 2, 2),
            "xl": lax.rem(index, 2),
        }

    def remote(source, target, send, recv, where):
        return pltpu.make_async_remote_copy(
            src_ref=source, dst_ref=target, send_sem=send, recv_sem=recv,
            device_id=where, device_id_type=MESH,
        )

    barrier = pltpu.get_barrier_semaphore()

    @pl.loop(1, 2 * COUNT)
    def _(i):
        other = lax.rem(me * 2 + core + i, 2 * COUNT)
        pl.semaphore_signal(
            barrier, inc=1, device_id={**device(other // 2), "core": lax.rem(other, 2)},
            device_id_type=MESH,
        )

    own_rows = pltpu.make_async_copy(shard, rows_in.at[core, pl.ds(HALO, slots)], token_sem)
    own_rows.start()
    end_copies = [
        pltpu.make_async_copy(
            shard.at[pl.ds((i + 1) * BLOCK - HALO, HALO)], ends.at[i], end_sem.at[i]
        )
        for i in range(slots // BLOCK)
    ]
    for copy in end_copies:
        copy.start()

    t = LANES
    for side in range(2):
        for other in range(2):
            index = side * 2 + other
            value, gate = model + other * inner, other * inner
            if side == 0:
                maps = 2 * model + other * t
                raw = 2 * model + 2 * t
                pieces[index, :, 0:t] = shard_ref[:, maps : maps + t]
                pieces[index, :, t : 2 * t] = jnp.zeros((shard_ref.shape[0], t), BF16)
                pieces[index, :, t : t + 2 * head_count] = shard_ref[:, raw : raw + 2 * head_count]
                pieces[index, :, 2 * t : 3 * t] = shard_ref[:, value : value + t]
                pieces[index, :, 3 * t : 6 * t] = shard_ref[:, value + 4 * t : value + 7 * t]
                pieces[index, :, 6 * t :] = shard_ref[:, gate : gate + 5 * t]
            else:
                pieces[index, :, 0 : 3 * t] = shard_ref[:, value + t : value + 4 * t]
                pieces[index, :, 3 * t : 6 * t] = shard_ref[:, value + 7 * t : value + 10 * t]
                pieces[index, :, 6 * t :] = shard_ref[:, gate + 5 * t : gate + 10 * t]

    block_count = bounds_ref[0, 0, 1] - bounds_ref[0, 0, 0]
    live[core] = jnp.full((8, LANES), (block_count * BLOCK).astype(F32))
    heads[...] = jnp.zeros_like(heads)
    for i, ref in enumerate((dt_ref, decay_ref, skip_ref)):
        heads[i : i + 1, 0 : 2 * head_count] = ref[...]
    both = heads[...]
    mine = jnp.where(core == 0, both, pltpu.roll(both, LANES - head_count, 1))
    lane8 = lax.broadcasted_iota(jnp.int32, (8, LANES), 1)
    heads[...] = jnp.where(lane8 < head_count, mine, 0.0)
    pl.semaphore_wait(barrier, 2 * COUNT - 1)

    my_part = xl * 2 + core

    def part_copy(step):
        target = lax.rem(my_part + step, 4)
        return remote(
            pieces.at[target], parts.at[my_part], part_send.at[step], part_recv.at[step],
            {"xl": target // 2, "core": lax.rem(target, 2)},
        )

    def part_arrival(step):
        source = lax.rem(my_part + 4 - step, 4)
        return remote(
            pieces.at[0], parts.at[source], part_send.at[step], part_recv.at[step], partner
        )

    for step in (1, 2, 3):
        part_copy(step).start()
    parts[my_part] = pieces[my_part]

    rows_copy = remote(
        shard, rows_in.at[core, pl.ds(HALO, slots)], token_send, token_recv, partner
    )
    live_copy = remote(live.at[core], live.at[core], live_send, live_recv, partner)
    live_copy.start()
    for copy in end_copies:
        copy.wait()
    chosen = ends[0].astype(F32)
    for i in range(1, slots // BLOCK):
        chosen = jnp.where(block_count == i + 1, ends[i].astype(F32), chosen)
    edge[...] = chosen.astype(BF16)

    def edge_copy(side):
        return remote(
            edge, rows_in.at[core, pl.ds(0, HALO)], edge_send.at[side], edge_recv.at[core],
            {**device(me + 1), "core": side},
        )

    @pl.when(me < COUNT - 1)
    def _():
        for side in range(2):
            edge_copy(side).start()

    @pl.when(me == 0)
    def _():
        rows_in[:, 0:HALO, :] = jnp.zeros((2, HALO, model), BF16)

    for step in (1, 2, 3):
        part_arrival(step).wait_recv()
    block = jnp.concatenate([parts[i].astype(F32) for i in range(4)], axis=0).astype(BF16)
    for tile in range(top.shape[0]):
        lanes = slice(tile * LANES, (tile + 1) * LANES)
        top[tile, y, z, xh, xl] = block[0:CUT, lanes]
        bottom[tile, y, z, xh, xl] = block[CUT:, lanes]

    near = lambda axis, step: lax.rem(here[axis] + step + 4, 4)

    def along(axis, step):
        coordinate = near(axis, step)
        if axis == "x":
            return {"xh": coordinate // 2, "xl": lax.rem(coordinate, 2)}
        return {axis: coordinate}

    def region(group, color, half, spot):
        wy, wz, wx = (spot[axis] for axis in ("y", "z", "x"))
        high, low = (slice(None), slice(None)) if wx is None else (wx // 2, lax.rem(wx, 2))
        wy = slice(None) if wy is None else wy
        wz = slice(None) if wz is None else wz
        first, tiles = GROUPS[group][color]
        first = first if tiles == 1 else pl.ds(first, tiles)
        ref = bottom if half == (group != 1) else top
        return ref.at[first, wy, wz, high, low]

    def spot_of(color, stage, coordinate):
        spot = dict(here)
        for axis in ORDERS[color][:stage]:
            spot[axis] = None
        spot[ORDERS[color][stage]] = coordinate
        return spot

    def ring_copy(group, color, stage, slot):
        offset, half, step = SLOTS[slot]
        axis = ORDERS[color][stage]
        target = region(group, color, half, spot_of(color, stage, near(axis, offset)))
        return remote(
            target, target, gather_send.at[group, color, stage, slot],
            gather_recv.at[group, color, stage, slot], along(axis, step),
        )

    def ring_arrival(group, color, stage, slot):
        offset, half, step = SLOTS[slot]
        axis = ORDERS[color][stage]
        target = region(group, color, half, spot_of(color, stage, near(axis, offset - step)))
        return remote(
            target, target, gather_send.at[group, color, stage, slot],
            gather_recv.at[group, color, stage, slot], along(axis, step),
        )

    def ring_start(group, stage):
        for color in range(3):
            if stage:
                for slot in (1, 2, 4, 5):
                    ring_arrival(group, color, stage - 1, slot).wait_recv()
            for slot in (0, 3, 1, 4):
                ring_copy(group, color, stage, slot).start()

    def ring_forward(group, stage):
        for color in range(3):
            ring_arrival(group, color, stage, 0).wait_recv()
            ring_copy(group, color, stage, 2).start()
            ring_arrival(group, color, stage, 3).wait_recv()
            ring_copy(group, color, stage, 5).start()

    def ring_finish(group):
        for color in range(3):
            for slot in (1, 2, 4, 5):
                ring_arrival(group, color, 2, slot).wait_recv()

    ring_start(0, 0)
    rows_copy.start()
    ring_forward(0, 0)
    ring_start(0, 1)
    ring_start(1, 0)
    lane = lax.broadcasted_iota(jnp.int32, (LANES, inner), 1)
    first = lax.broadcasted_iota(jnp.int32, (LANES, inner), 0) * (inner // head_count)
    ones = jnp.where(
        jnp.logical_and(lane >= first, lane < first + inner // head_count), 1.0, 0.0
    ).astype(BF16)
    rows = lax.broadcasted_iota(jnp.int32, (CHUNK, LANES), 0)
    columns = lax.broadcasted_iota(jnp.int32, (CHUNK, LANES), 1)
    below = jnp.where(rows >= columns, 1.0, 0.0).astype(BF16)
    for i in range(3):
        spread_ref[i * LANES : (i + 1) * LANES, :] = ones
        tri_ref[:, i * LANES : (i + 1) * LANES] = below
    ring_forward(0, 1)
    ring_forward(1, 0)
    ring_start(0, 2)
    ring_start(1, 1)
    skips[...] = dot(jnp.concatenate(split3(heads[...]), axis=1), spread_ref[...])
    ring_forward(0, 2)
    ring_forward(1, 1)
    ring_start(1, 2)
    ring_start(2, 0)
    own_rows.wait()
    rows_copy.wait_send()
    remote(
        shard, rows_in.at[1 - core, pl.ds(HALO, slots)], token_send, token_recv, partner
    ).wait_recv()
    remote(live.at[core], live.at[1 - core], live_send, live_recv, partner).wait_recv()

    @pl.when(me > 0)
    def _():
        for side in range(2):
            remote(
                edge, rows_in.at[side, pl.ds(0, HALO)], edge_send.at[side], edge_recv.at[side],
                partner,
            ).wait_recv()

    ring_finish(0)
    ring_forward(2, 0)
    ring_start(2, 1)

    def matrix(tile):
        pair = [
            jnp.concatenate(
                [
                    top[tile, :, :, :, i].reshape(-1, CUT, LANES),
                    bottom[tile, :, :, :, i].reshape(-1, model // 32 - CUT, LANES),
                ],
                axis=1,
            ).reshape(model, LANES)
            for i in range(2)
        ]
        return jnp.concatenate(pair, axis=1)

    def both_lanes(ref, row, starts):
        return jnp.concatenate([ref[row : row + 1, pl.ds(start, LANES)] for start in starts], axis=1)

    def project_mixed(group, seq, color):
        result = dot(rows_in[seq], matrix(GROUPS[group][0][0] + color)).astype(BF16)
        tiles = [group * 6 + color, group * 6 + color + 3]
        if group == 0:
            raw_all[seq, jnp.where(color == 1, 1, 0)] = result[HALO:, 0:LANES]
        spots = [
            jnp.where(
                tile == 0, model // LANES + core, core * (inner // LANES) + jnp.maximum(tile - 2, 0)
            )
            for tile in tiles
        ]
        lanes = [pl.multiple_of(spot * LANES, LANES) for spot in spots]
        mixed = result.astype(F32)
        conv = jnp.concatenate([bias_ref[pl.ds(spot, 1), :] for spot in spots], axis=1)
        for k in range(4):
            conv = conv + both_lanes(taps_ref, k, lanes) * mixed[HALO - 3 + k : HALO - 3 + k + slots]
        act = (conv * jax.nn.sigmoid(conv)).astype(BF16)
        for i, tile in enumerate(tiles):
            act_all[seq, :, pl.ds(pl.multiple_of(tile * LANES, LANES), LANES)] = act[
                :, i * LANES : (i + 1) * LANES
            ]

    def project_gate(first, last):
        @pl.loop(first, last)
        def _(i):
            seq = i // 5
            color = lax.rem(i, 5)
            result = dot(rows_in[seq, HALO:, :], matrix(GROUPS[2][0][0] + color))
            for half in range(2):
                tile = pl.ds(pl.multiple_of((half * 5 + color) * LANES, LANES), LANES)
                act_all[seq, :, tile] = result[:, half * LANES : (half + 1) * LANES].astype(BF16)

    map_copy = remote(act_all.at[:, :, pl.ds(0, LANES)], far_map, map_send, map_recv, partner)

    @pl.loop(0, 6)
    def _(i):
        project_mixed(0, lax.rem(i, 2), i // 2)

        @pl.when(i == 1)
        def _():
            ring_forward(1, 2)
            ring_forward(2, 1)

        @pl.when(i == 4)
        def _():
            map_copy.start()
            ring_start(2, 2)

    ring_finish(1)

    def slice_of(ref, seq, k):
        row = pl.multiple_of(k // 2 * 8, 8)
        column = pl.multiple_of(lax.rem(k, 2) * wide, LANES)
        return ref.at[seq, pl.ds(row, 8), pl.ds(column, wide)]

    my_k = (y * 4 + z) * 2 + xh
    my_seq = lax.rem(y + z + xl, 2)

    def owner(seq, k):
        oy, oz = k // 8, lax.rem(k // 2, 4)
        return {"y": oy, "z": oz, "xh": lax.rem(k, 2), "xl": lax.rem(seq + oy + oz, 2)}

    def piece(seq, k, slot):
        return remote(
            slice_of(state, seq, k), arrived.at[slot], piece_send.at[seq * OWNERS + k],
            piece_recv.at[slot], owner(seq, k),
        )

    def decay_copy(seq, k, slot):
        return remote(
            total.at[seq], decays.at[slot], decay_send.at[seq * OWNERS + k],
            decay_recv.at[slot], owner(seq, k),
        )

    def back(index, seq, k):
        return remote(
            starts.at[index], slice_of(incoming, seq, k), back_send.at[index],
            back_recv.at[seq * OWNERS + k], device(index),
        )

    def scan_chunk(seq, chunk):
        row0 = pl.multiple_of(chunk * CHUNK, CHUNK)
        window = pl.ds(row0, CHUNK)
        near_map = act_all[seq, window, 0:LANES]
        other_map = far_map[seq, window, :]
        in_map = jnp.where(core == 0, near_map, other_map)
        out_map = jnp.where(core == 0, other_map, near_map)
        value = act_all[seq, window, 2 * LANES :]

        raw = raw_all[seq, 1, window, :].astype(F32)
        raw = jnp.where(core == 0, raw, pltpu.roll(raw, LANES - head_count, 1))
        raw = raw + heads[0:1, :]
        tail = jnp.exp(-jnp.abs(raw))
        series = tail * (1.0 - tail * (0.5 - tail * (1.0 / 3.0 - 0.25 * tail)))
        step = jnp.maximum(raw, 0.0) + jnp.where(tail < 0.01, series, jnp.log(1.0 + tail))
        step = jnp.where((rows + row0).astype(F32) < live[seq, 0:1, :], step, 0.0)
        log_decay = -(step * heads[1:2, :]) * LOG2E
        cum = dot(tri_ref[...], jnp.concatenate(split3(log_decay), axis=0))
        shifted = jnp.where(step > 0.0, cum - jnp.log(step) * LOG2E, 1e30).T
        causal = rows >= columns
        scores = lax.dot_general(
            out_map, in_map, (((1,), (1,)), ((), ())), preferred_element_type=F32
        )
        before = state[seq]
        growth = dot(jnp.concatenate(split3(jnp.exp2(cum)), axis=1), spread_ref[...])
        reach = dot(
            jnp.concatenate([out_map, out_map], axis=1), jnp.concatenate(split2(before), axis=0)
        )
        base = growth * reach + skips[2:3, :] * value.astype(F32)
        left = columns < LANES // 2
        zero = jnp.zeros((CHUNK, LANES), BF16)
        for tile in range(inner // LANES):
            lanes = slice(tile * LANES, (tile + 1) * LANES)
            result = base[:, lanes]
            for side in range(2):
                head = tile * 2 + side
                reached = jnp.where(
                    causal, cum[:, head : head + 1] - shifted[head : head + 1, :], -1e30
                )
                mixing = jnp.exp2(reached) * scores
                kept = jnp.where(left if side == 0 else ~left, value[:, lanes], zero)
                result = result + dot(
                    jnp.concatenate(split2(mixing), axis=1), jnp.concatenate([kept, kept], axis=0)
                )
            y_all[seq, pl.ds(row0, CHUNK), lanes] = result

        last = cum[CHUNK - 1 : CHUNK, :]
        to_end = jnp.exp2(last - cum) * step
        weighted = value.astype(F32) * dot(
            jnp.concatenate(split3(to_end), axis=1), spread_ref[...]
        )
        added = lax.dot_general(
            jnp.concatenate([in_map, in_map], axis=0),
            jnp.concatenate(split2(weighted), axis=0),
            (((0,), (0,)), ((), ())),
            preferred_element_type=F32,
        )
        state[seq] = growth[CHUNK - 1 : CHUNK, :] * before + added
        map_all[seq, pl.ds(row0, CHUNK), :] = out_map
        cum_all[seq, pl.ds(row0, CHUNK), :] = cum + total[seq]
        total[seq] = total[seq] + last

    def compose_all():
        @pl.loop(1, COUNT)
        def _(i):
            peer = lax.rem(me + i, COUNT)
            decay_copy(my_seq, my_k, peer).wait_recv()
            piece(my_seq, my_k, peer).wait_recv()

        column = pl.multiple_of(lax.rem(my_k, 2) * wide, LANES)
        decay = jnp.exp2(decays[...].reshape(COUNT, LANES))
        factors[...] = dot(
            jnp.concatenate(split3(decay), axis=1), spread_ref[:, pl.ds(column, wide)]
        )

        def compose(index, carry):
            starts[index] = carry
            return factors[pl.ds(index, 1), :] * carry + arrived[index]

        lax.fori_loop(0, COUNT, compose, jnp.zeros((8, wide), F32))

        @pl.loop(1, COUNT)
        def _(i):
            back(lax.rem(me + i, COUNT), my_seq, my_k).start()

        slice_of(incoming, my_seq, my_k)[...] = starts[me]

    state[...] = jnp.zeros_like(state)
    total[...] = jnp.zeros_like(total)

    @pl.loop(0, 2)
    def _(seq):
        @pl.loop(0, 3)
        def _(color):
            project_mixed(1, seq, color)

        @pl.when(seq == 0)
        def _():
            map_copy.wait()

        @pl.loop(0, slots // CHUNK)
        def _(chunk):
            scan_chunk(seq, chunk)

            @pl.when(jnp.logical_and(seq == 0, chunk == 1))
            def _():
                ring_forward(2, 2)

        @pl.loop(0, OWNERS)
        def _(i):
            k = lax.rem(my_k + i, OWNERS)
            mine = jnp.logical_and(i == 0, seq == my_seq)

            @pl.when(jnp.logical_not(mine))
            def _():
                decay_copy(seq, k, me).start()
                piece(seq, k, me).start()

            @pl.when(mine)
            def _():
                arrived[me] = slice_of(state, seq, k)[...]
                decays[me] = total[seq]

    ring_finish(2)
    project_gate(0, 10)
    compose_all()

    def square_copy(seq):
        return remote(
            square.at[seq], far_square.at[seq], square_send.at[seq], square_recv.at[seq], partner
        )

    @pl.loop(0, 2)
    def _(seq):
        @pl.loop(0, slots // CHUNK)
        def _(chunk):
            row0 = pl.multiple_of(chunk * CHUNK, CHUNK)
            here_rows = pl.ds(row0, CHUNK)
            growth = dot(
                jnp.concatenate(split3(jnp.exp2(cum_all[seq, here_rows, :])), axis=1),
                spread_ref[...],
            )
            gate = act_all[seq, here_rows, 0:inner].astype(F32)
            gate = gate * jax.nn.sigmoid(gate)
            y_all[seq, here_rows, :] = y_all[seq, here_rows, :] * gate
            lift[seq, here_rows, :] = growth * gate

    def gate_sequence(seq):
        @pl.loop(0, OWNERS)
        def _(k):
            @pl.when(jnp.logical_not(jnp.logical_and(k == my_k, my_seq == seq)))
            def _():
                back(me, seq, k).wait_recv()

        start = jnp.concatenate(split2(incoming[seq]), axis=0)

        @pl.loop(0, slots // CHUNK)
        def _(chunk):
            row0 = pl.multiple_of(chunk * CHUNK, CHUNK)
            here_rows = pl.ds(row0, CHUNK)
            out_map = map_all[seq, here_rows, :]
            reach = dot(jnp.concatenate([out_map, out_map], axis=1), start)
            gated = y_all[seq, here_rows, :] + lift[seq, here_rows, :] * reach
            y_all[seq, here_rows, :] = gated
            square[seq, here_rows, :] = jnp.broadcast_to(
                jnp.sum(gated * gated, axis=1, keepdims=True), (CHUNK, LANES)
            )

        square_copy(seq).start()

    def out_copy(piece):
        part = pl.ds(piece * BLOCK, BLOCK)
        return remote(
            staged.at[part], out_ref.at[part, pl.ds(core_lane, inner)], out_send.at[piece],
            out_recv.at[piece], partner,
        )

    gain = jnp.concatenate(
        [gain_ref[pl.ds(core * (inner // LANES) + i, 1), :] for i in range(inner // LANES)], axis=1
    )

    def finish_sequence(seq):
        square_copy(seq).wait_recv()

        def normed(row0):
            here_rows = pl.ds(row0, CHUNK)
            mean = (square[seq, here_rows, 0:1] + far_square[seq, here_rows, 0:1]) / model
            result = y_all[seq, here_rows, :] * lax.rsqrt(mean + 1e-05) * gain
            kept = (rows[:, 0:1] + row0).astype(F32) < live[seq, 0:1, 0:1]
            return jnp.where(kept, result, 0.0).astype(BF16)

        @pl.when(core == seq)
        def _():
            @pl.loop(0, slots // CHUNK)
            def _(chunk):
                row0 = pl.multiple_of(chunk * CHUNK, CHUNK)
                out_ref[pl.ds(row0, CHUNK), pl.ds(core_lane, inner)] = normed(row0)

        @pl.when(core != seq)
        def _():
            for piece in range(slots // BLOCK):
                @pl.loop(0, BLOCK // CHUNK)
                def _(chunk):
                    row0 = pl.multiple_of(piece * BLOCK + chunk * CHUNK, CHUNK)
                    staged[pl.ds(row0, CHUNK), :] = normed(row0)

                out_copy(piece).start()

    for seq in range(2):
        gate_sequence(seq)
    for seq in range(2):
        finish_sequence(seq)

    for step in (1, 2, 3):
        part_copy(step).wait_send()
    live_copy.wait_send()

    @pl.when(me < COUNT - 1)
    def _():
        for side in range(2):
            edge_copy(side).wait_send()

    for group in range(3):
        for stage in range(3):
            for color in range(3):
                for slot in range(6):
                    ring_copy(group, color, stage, slot).wait_send()

    @pl.loop(0, 2 * OWNERS)
    def _(i):
        seq = i // OWNERS
        k = lax.rem(i, OWNERS)

        @pl.when(jnp.logical_not(jnp.logical_and(k == my_k, my_seq == seq)))
        def _():
            piece(seq, k, me).wait_send()
            decay_copy(seq, k, me).wait_send()

    @pl.loop(1, COUNT)
    def _(i):
        back(lax.rem(me + i, COUNT), my_seq, my_k).wait_send()

    for seq in range(2):
        square_copy(seq).wait_send()
    far_lane = pl.multiple_of((1 - core) * inner, LANES)
    for piece in range(slots // BLOCK):
        out_copy(piece).wait_send()
        part = pl.ds(piece * BLOCK, BLOCK)
        remote(
            staged.at[part], out_ref.at[part, pl.ds(far_lane, inner)], out_send.at[piece],
            out_recv.at[piece], partner,
        ).wait_recv()


def local(
    tokens, bounds, in_weight, conv_weight, conv_bias, dt_bias, decay_rate, skip_gain, norm_gain
):
    slots, model = tokens.shape[1:]
    inner = model // 2
    rows = in_weight.shape[0]
    padded = slots + HALO
    columns = 11 * LANES
    vmem = pl.BlockSpec(memory_space=pltpu.VMEM)
    dma = pltpu.SemaphoreType.DMA
    out = pl.pallas_call(
        layer_kernel,
        out_shape=jax.ShapeDtypeStruct((slots, model), BF16),
        in_specs=[
            pl.BlockSpec(memory_space=pltpu.SMEM), pl.BlockSpec(memory_space=pl.ANY),
        ] + [vmem] * 7,
        out_specs=vmem,
        scratch_shapes=[
            pltpu.VMEM((2, padded, model), BF16),
            pltpu.VMEM((columns // LANES, 4, 4, 2, 2, CUT, LANES), BF16),
            pltpu.VMEM((columns // LANES, 4, 4, 2, 2, 4 * rows - CUT, LANES), BF16),
            pltpu.VMEM((2, slots, 12 * LANES), BF16),
            pltpu.VMEM((2, 2, slots, LANES), BF16),
            pltpu.VMEM((3 * LANES, inner), BF16),
            pltpu.VMEM((CHUNK, 3 * LANES), BF16),
            pltpu.VMEM((8, LANES), F32),
            pltpu.VMEM((8, inner), F32),
            pltpu.VMEM((4, rows, columns), BF16),
            pltpu.VMEM((slots // BLOCK, HALO, model), BF16),
            pltpu.VMEM((HALO, model), BF16),
            pltpu.VMEM((2, slots, LANES), BF16),
            pltpu.VMEM((2, slots, inner), F32),
            pltpu.VMEM((2, slots, LANES), BF16),
            pltpu.VMEM((2, slots, LANES), F32),
            pltpu.VMEM((2, LANES, inner), F32),
            pltpu.VMEM((2, 1, LANES), F32),
            pltpu.VMEM((4, rows, columns), BF16),
            pltpu.VMEM((COUNT, 8, inner // 2), F32),
            pltpu.VMEM((COUNT, 8, inner // 2), F32),
            pltpu.VMEM((COUNT, 1, LANES), F32),
            pltpu.VMEM((COUNT, inner // 2), F32),
            pltpu.VMEM((2, LANES, inner), F32),
            pltpu.VMEM((2, slots, LANES), F32),
            pltpu.VMEM((2, slots, LANES), F32),
            pltpu.VMEM((slots, inner), BF16),
            pltpu.VMEM((2, 8, LANES), F32),
            pltpu.VMEM((2, slots, inner), F32),
            dma((slots // BLOCK,)),
            dma((4,)), dma((4,)),
            dma, dma, dma,
            dma((2,)), dma((2,)),
            dma, dma,
            dma((3, 3, 3, 6)), dma((3, 3, 3, 6)),
            dma, dma,
            dma((COUNT,)), dma((COUNT,)), dma((COUNT,)), dma((COUNT,)),
            dma((COUNT,)), dma((COUNT,)),
            dma((2,)), dma((2,)),
            dma((slots // BLOCK,)), dma((slots // BLOCK,)),
        ],
        compiler_params=pltpu.CompilerParams(
            collective_id=0, has_side_effects=True, vmem_limit_bytes=67043328
        ),
        name="layer",
    )(
        bounds, tokens, in_weight, conv_weight, conv_bias.reshape(-1, LANES), dt_bias[None], decay_rate[None],
        skip_gain[None], norm_gain.reshape(-1, LANES),
    )
    return out[None]


def solution(mesh):
    split = Mesh(mesh.devices.reshape(4, 4, 2, 2, 2), AXES + ("core",))
    return jax.shard_map(
        local,
        mesh=split,
        in_specs=(
            P("core", AXES, None),
            P("core", AXES, None),
            P(AXES + ("core",), None),
            P(), P(), P(), P(), P(), P(),
        ),
        out_specs=P("core", AXES, None),
        check_vma=False,
    )
```
